32 devices in a mesh: seq: 32 (over z, y, x, core).
Axes of the slice: x: 2, y: 2, z: 4, core: 2. Of those that a mesh axis runs over, the one named last changes fastest.
Arguments:
- residual: bfloat16 [4096, 2560], P('seq'), may hold values from -6 to 6
- queries: bfloat16 [4096, 2560], P('seq'), may hold values from -5 to 5, as said below
- keys: bfloat16 [4096, 512], P('seq'), may hold values from -5 to 5
- values: bfloat16 [4096, 512], P('seq'), may hold values from -6 to 6
- out_proj: bfloat16 [2560, 2560], P(None, 'seq'), may hold values from -0.125 to 0.125
- norm_gain: float32 [2560], replicated, may hold values from 0.25 to 1.75
- expert_in: bfloat16 [2560, 2, 106496], P(None, None, 'seq'), may hold values from -0.125 to 0.125
- expert_down: bfloat16 [106496, 2560], P('seq'), may hold values from -0.15625 to 0.15625
- routes: int32 [4096, 2], P('seq'), may hold values from 0 to 63, all different within a row
- gate_ints: int32 [4096, 2], P('seq'), may hold values from 1 to 1023
- modality: int32 [4096], P('seq'), may hold values 0 or 1
- capacity: int32 [64, 2], replicated, may hold values from 1 to 2, as said below
Outputs:
- attended: bfloat16 [4096, 2560], P('seq')
- expert_mix: bfloat16 [4096, 2560], P('seq')
The draws below stay inside these ranges and needn't reach their ends.
Inputs may be any that keep to these rules, and one draw needn't show every extreme that they name: `queries` and `keys`: every element lies between -5 and 5. `routes`: each token names two different experts. `capacity`: some entry equals 2.
All inputs are finite; a program needn't handle non-finite values. No bound on the sum of `modality` on one device may be relied on, other than what follows from the above.
Results may differ from the reference program's by a relative error of at most 0.0086.
Values may be sent and summed in bfloat16 or wider, within the bound.
A program may use at most 192 MiB of HBM per device.

```python
import math
import jax
import jax.numpy as jnp
from jax import lax

D = 2560
HEADS = 20
KV_HEADS = 4
HEAD = 128
WINDOW = 1024
EXPERTS = 64
FF = 1664
TOK_DEV = 128
CAP = 2
TOKENS = 4096
N_SEQ = 32


def draw_queries(key, part):
    drawn = jnp.clip(jax.random.normal(jax.random.fold_in(key, 3), (TOKENS, HEADS * HEAD), jnp.float32), -5.0, 5.0)
    return drawn.astype(jnp.bfloat16)


def draw_keys(key, part):
    drawn = jnp.clip(jax.random.normal(jax.random.fold_in(key, 4), (TOKENS, KV_HEADS * HEAD), jnp.float32), -5.0, 5.0)
    return drawn.astype(jnp.bfloat16)


def draw_capacity(key, part):
    cap_table = jax.random.randint(jax.random.fold_in(key, 21), (EXPERTS * 2,), 1, CAP + 1)
    full_spot = jax.random.randint(jax.random.fold_in(key, 22), (), 0, EXPERTS * 2)
    cap_table = jnp.where(jnp.arange(EXPERTS * 2) == full_spot, CAP, cap_table)
    return cap_table.reshape(EXPERTS, 2).astype(jnp.int32)


def set_ends(values, own_key, least, largest):
    longest = values.shape.index(max(values.shape))
    spots = []
    for shift in (0, 1):
        where = [jax.random.randint(jax.random.fold_in(own_key, axis), (), 0, length) for axis, length in enumerate(values.shape)]
        where[longest] = (where[longest] + shift) % values.shape[longest]
        spots.append(tuple(where))
    return values.at[spots[0]].set(least).at[spots[1]].set(largest)


def steps_of(own_key, dims, split, smallest, high):
    level = 1.0
    for axis_at, parts in split:
        heights = jax.random.uniform(jax.random.fold_in(jax.random.fold_in(own_key, 6), axis_at), (parts,), jnp.float32, smallest / len(split), high / len(split))
        level = level * jnp.repeat(jnp.exp(heights), dims[axis_at] // parts).reshape((-1,) + (1,) * (len(dims) - 1 - axis_at))
    return level


def picks_of(stream_key, rows, amount, top, lift):
    ranking = jax.random.permutation(jax.random.fold_in(stream_key, 1), amount)
    pull = ranking
    for power in range(3):
        pull = pull * pull // amount
    pull = pull * lift // amount
    lots = jax.random.randint(jax.random.fold_in(stream_key, 2), (rows, amount), 0, 4096) + pull
    fixed_rows = jax.random.permutation(jax.random.fold_in(stream_key, 3), rows)[jnp.arange(amount) % rows]
    lots = jnp.where(jnp.arange(rows)[:, None] == fixed_rows[None, :], 1 << 14, lots)
    score = lots * amount + jnp.arange(amount)
    return lax.top_k(score.astype(jnp.int32), top)[1].astype(jnp.int32)


def bell_draw(own_key, shape, deviation, bound, cuts=(), held_as=jnp.bfloat16):
    result = deviation * jax.random.normal(own_key, shape, jnp.float32)
    if cuts:
        result = result * steps_of(own_key, shape, cuts, -0.22, 0.18)
    return jnp.clip(result, -bound, bound).astype(held_as)


def setup_inputs(seed: int = 0) -> dict:
    key_list = jax.random.split(jax.random.key(seed), 13)
    return {
        "residual": bell_draw(key_list[0], (TOKENS, D), 1.0, 6.0, ((0, 32),)),
        "queries": draw_queries(jax.random.fold_in(key_list[12], 71), 0),
        "keys": draw_keys(jax.random.fold_in(key_list[12], 71), 0),
        "values": bell_draw(key_list[3], (TOKENS, KV_HEADS * HEAD), 1.0, 6.0, ((0, 32),)),
        "out_proj": bell_draw(key_list[4], (HEADS * HEAD, D), (HEADS * HEAD) ** -0.5, 0.125, ((1, 32),)),
        "norm_gain": jnp.clip(1.0 + 0.15 * jax.random.normal(key_list[5], (D,), jnp.float32), 0.25, 1.75),
        "expert_in": bell_draw(key_list[6], (D, 2, EXPERTS * FF), D ** -0.5, 0.125, ((2, 32),)),
        "expert_down": bell_draw(key_list[7], (EXPERTS * FF, D), FF ** -0.5, 0.15625, ((0, 32),)),
        "routes": picks_of(key_list[8], TOKENS, EXPERTS, 2, 512),
        "gate_ints": set_ends(jax.random.randint(key_list[9], (TOKENS, 2), 1, 1024), jax.random.fold_in(key_list[9], 1), 1, 1023).astype(jnp.int32),
        "modality": set_ends((jax.random.randint(key_list[10], (TOKENS,), 0, 2) < 1).astype(jnp.int32), jax.random.fold_in(key_list[10], 1), 0, 1),
        "capacity": draw_capacity(jax.random.fold_in(key_list[12], 71), 0),
    }


def attend(queries, keys, values):
    row_total = queries.shape[0]
    q_group = HEADS // KV_HEADS
    q_block = math.gcd(row_total, 512)
    q_blocks = queries.reshape(row_total // q_block, q_block, KV_HEADS, q_group, HEAD)
    keys_padded = jnp.pad(keys, ((WINDOW, 0), (0, 0))).reshape(row_total + WINDOW, KV_HEADS, HEAD)
    values_padded = jnp.pad(values, ((WINDOW, 0), (0, 0))).reshape(row_total + WINDOW, KV_HEADS, HEAD)

    def one_block(block_idx):
        first_row = (block_idx * q_block).astype(jnp.int32)
        q_here = lax.dynamic_index_in_dim(q_blocks, block_idx, 0, keepdims=False).astype(jnp.float32)
        k_here = lax.dynamic_slice_in_dim(keys_padded, first_row, q_block + WINDOW, 0).astype(jnp.float32)
        v_here = lax.dynamic_slice_in_dim(values_padded, first_row, q_block + WINDOW, 0).astype(jnp.float32)
        scores = jnp.einsum('qhgd,khd->hgqk', q_here, k_here) * HEAD ** (-0.5)
        q_pos = first_row + jnp.arange(q_block, dtype=jnp.int32)
        k_pos = first_row - WINDOW + jnp.arange(q_block + WINDOW, dtype=jnp.int32)
        visible = (k_pos[None, :] <= q_pos[:, None]) & (k_pos[None, :] > q_pos[:, None] - WINDOW) & (k_pos[None, :] >= 0)
        scores = jnp.where(visible, scores, -jnp.inf)
        row_max = lax.optimization_barrier(jnp.max(scores, -1, keepdims=True))
        weights_raw = jnp.exp(scores - row_max)
        probs_bf = (weights_raw / lax.optimization_barrier(jnp.sum(weights_raw, -1, keepdims=True))).astype(jnp.bfloat16)
        context = jnp.einsum('hgqk,khd->qhgd', probs_bf.astype(jnp.float32), v_here)
        return context.reshape(q_block, HEADS * HEAD).astype(jnp.bfloat16)
    mapped = lax.map(one_block, jnp.arange(row_total // q_block, dtype=jnp.int32))
    return mapped.reshape(row_total, HEADS * HEAD)

def experts_ref(normed, expert_in, expert_down, routes, gate_ints, modality, capacity):
    split_ways = max(1, N_SEQ // EXPERTS)
    slot_count = 2 * CAP
    expert = routes.reshape(N_SEQ, TOK_DEV * 2)
    mode_flag = jnp.repeat(modality, 2).reshape(N_SEQ, TOK_DEV * 2)
    slot_key = expert * 2 + mode_flag
    onehot = (slot_key[:, :, None] == jnp.arange(2 * EXPERTS, dtype=jnp.int32)[None, None, :]).astype(jnp.int32)
    before = jnp.cumsum(onehot, axis=1) - onehot
    rank_in = lax.optimization_barrier(jnp.sum(before * onehot, -1))
    limit_of = capacity.reshape(-1)[slot_key]
    kept_mask = rank_in < limit_of
    source = jnp.arange(N_SEQ, dtype=jnp.int32)[:, None]
    place_at = expert * (N_SEQ * slot_count) + source * slot_count + mode_flag * CAP + rank_in
    outside = EXPERTS * N_SEQ * slot_count
    place_at = jnp.where(kept_mask, place_at, outside).astype(jnp.int32)
    token_ids = jnp.repeat(jnp.arange(TOKENS, dtype=jnp.int32), 2)
    slot_table = jnp.full((outside,), TOKENS, jnp.int32).at[place_at.reshape(-1)].set(token_ids, mode='drop')
    slot_table = slot_table.reshape(EXPERTS, N_SEQ * slot_count)
    padded = jnp.concatenate([normed, jnp.zeros((1, D), jnp.bfloat16)], 0)
    part_width = FF // split_ways

    def one_expert(expert_id):
        picked_rows = padded[slot_table[expert_id]]
        zero_at = jnp.zeros((), jnp.int32)
        first_col = (expert_id * FF).astype(jnp.int32)
        weights_here = lax.dynamic_slice(expert_in, (zero_at, zero_at, first_col), (D, 2, FF))
        gate_val = jnp.dot(picked_rows, weights_here[:, 0, :], preferred_element_type=jnp.float32)
        up_val = jnp.dot(picked_rows, weights_here[:, 1, :], preferred_element_type=jnp.float32)
        active = (jax.nn.silu(gate_val) * up_val).astype(jnp.bfloat16)
        down_rows = lax.dynamic_slice_in_dim(expert_down, first_col, FF, 0)
        summed = jnp.zeros((N_SEQ * slot_count, D), jnp.float32)
        for piece_idx in range(split_ways):
            lo_col = piece_idx * part_width
            partial_value = jnp.dot(active[:, lo_col:lo_col + part_width], down_rows[lo_col:lo_col + part_width], preferred_element_type=jnp.float32).astype(jnp.bfloat16)
            partial_value = lax.optimization_barrier(partial_value)
            summed = summed + partial_value.astype(jnp.float32)
        return summed.astype(jnp.bfloat16)
    expert_rows = lax.map(one_expert, jnp.arange(EXPERTS, dtype=jnp.int32))
    flat_rows = expert_rows.reshape(-1, D)
    pick_at = jnp.where(kept_mask, place_at, 0).reshape(-1).astype(jnp.int32)
    chosen_rows = flat_rows[pick_at].astype(jnp.float32).reshape(TOKENS, 2, D)
    gate_scale = jnp.where(kept_mask.reshape(TOKENS, 2), gate_ints.astype(jnp.float32) / 1024.0, 0.0)
    return lax.optimization_barrier(jnp.sum(gate_scale[:, :, None] * chosen_rows, 1)).astype(jnp.bfloat16)

def reference(residual, queries, keys, values, out_proj, norm_gain, expert_in, expert_down, routes, gate_ints, modality, capacity):
    context = attend(queries, keys, values)
    attended = jnp.dot(context, out_proj, preferred_element_type=jnp.float32).astype(jnp.bfloat16)
    attended = lax.optimization_barrier(attended)
    hidden = residual.astype(jnp.float32) + attended.astype(jnp.float32)
    normed = (hidden * lax.rsqrt(lax.optimization_barrier(jnp.mean(hidden * hidden, -1, keepdims=True)) + 1e-05) * norm_gain).astype(jnp.bfloat16)
    expert_mix = experts_ref(normed, expert_in, expert_down, routes, gate_ints, modality, capacity)
    return (attended, expert_mix)
```

```python
import functools
import math
import jax
import jax.numpy as jnp
from jax import lax
from jax.experimental import pallas as pl
from jax.experimental.pallas import tpu as pltpu
from jax.sharding import PartitionSpec as P

HEADS = 20
KV_HEADS = 4
HEAD = 128
WINDOW = 1024
EXPERTS = 64
CAP = 2
MESH = pl.DeviceIdType.MESH


def window_blocks(own, chips_back):
    count = lax.axis_size("seq")
    swap = [(source, source ^ 1) for source in range(count)]
    span = 2 * chips_back
    mine = {0: own}
    prev = lax.ppermute(own, "seq", [(s, s + span) for s in range(count - span)])
    mine[chips_back] = prev
    if count % span == 0:
        place = lax.rem(lax.axis_index("seq"), span) // 2
        for step in range(1, chips_back):
            payload = jnp.where(place + step < chips_back, own, prev)
            turn = [(s, s - s % span + (s % span + 2 * step) % span) for s in range(count)]
            mine[step] = lax.ppermute(payload, "seq", turn)
    else:
        for step in range(1, chips_back):
            mine[step] = lax.ppermute(own, "seq", [(s, s + 2 * step) for s in range(count - 2 * step)])
    other = {step: lax.ppermute(block, "seq", swap) for step, block in mine.items()}
    return mine, other


def attend_kernel(chips_back, rows, q_ref, *refs):
    out_ref = refs[-1]
    blocks = 2 * (chips_back + 1)
    k_refs, v_refs = refs[:blocks], refs[blocks : 2 * blocks]
    me = lax.axis_index("seq")
    core = lax.rem(me, 2)
    keys = jnp.concatenate([ref[...] for ref in k_refs], 0)
    vals = jnp.concatenate([ref[...] for ref in v_refs], 0)
    q_pos = me * rows + lax.broadcasted_iota(jnp.int32, (rows, rows), 0)
    lane = lax.broadcasted_iota(jnp.int32, (rows, rows), 1)
    bias = []
    for half in range(2):
        for step in range(chips_back + 1):
            block = (me - core) - 2 * step + (core if half == 0 else 1 - core)
            k_pos = block * rows + lane
            seen = (k_pos <= q_pos) & (k_pos > q_pos - WINDOW) & (k_pos >= 0)
            bias.append(jnp.where(seen, 0.0, -1e30))
    bias = jnp.concatenate(bias, 1)
    scale = HEAD ** (-0.5) * math.log2(math.e)
    for g in range(HEADS // KV_HEADS):
        q_one = q_ref[:, g * HEAD : (g + 1) * HEAD]
        scores = lax.dot_general(q_one, keys, (((1,), (1,)), ((), ())), preferred_element_type=jnp.float32)
        scores = scores * scale + bias
        weights = jnp.exp2(scores - jnp.max(scores, -1, keepdims=True))
        total = jnp.sum(weights, -1, keepdims=True)
        probs = (weights * (1.0 / total)).astype(jnp.bfloat16)
        mixed = jnp.dot(probs, vals, preferred_element_type=jnp.float32)
        out_ref[:, g * HEAD : (g + 1) * HEAD] = mixed.astype(jnp.bfloat16)


def attend(queries, mine, other, chips_back, part):
    rows = queries.shape[0]
    wide = HEADS // KV_HEADS * HEAD
    ordered = [mine[s] for s in range(chips_back + 1)] + [other[s] for s in range(chips_back + 1)]
    heads = KV_HEADS // 2
    first = part * heads
    k_spec = pl.BlockSpec((rows, HEAD), lambda h: (0, first + h))
    v_spec = pl.BlockSpec((rows, HEAD), lambda h: (0, KV_HEADS + first + h))
    q_spec = pl.BlockSpec((rows, wide), lambda h: (0, first + h))
    span = rows * len(ordered)
    return pl.pallas_call(
        functools.partial(attend_kernel, chips_back, rows),
        grid=(heads,),
        out_shape=jax.ShapeDtypeStruct((rows, heads * wide), jnp.bfloat16),
        in_specs=[q_spec] + [k_spec] * len(ordered) + [v_spec] * len(ordered),
        out_specs=pl.BlockSpec((rows, wide), lambda h: (0, h)),
        cost_estimate=pl.CostEstimate(
            flops=2 * HEADS * rows * span * HEAD, bytes_accessed=4 << 20, transcendentals=HEADS * rows * span // 2
        ),
        name="attend",
    )(queries, *ordered, *ordered)


def project(halves, out_proj):
    count = lax.axis_size("seq")
    rows = halves[0].shape[0]
    local = out_proj.shape[1]
    flip = [[(source, source ^ bits) for source in range(count)] for bits in range(4)]
    classes = [[s for s in range(count) if s % 4 == kind] for kind in range(4)]
    weights = lax.all_gather(out_proj.T, "seq", axis=0, tiled=True, axis_index_groups=classes)
    far = [lax.ppermute(half, "seq", flip[2]) for half in halves]
    near = [lax.ppermute(half, "seq", flip[1]) for half in halves]
    cross = [lax.ppermute(half, "seq", flip[1]) for half in far]

    def product(pieces):
        return lax.dot_general(
            weights, jnp.concatenate(pieces, 1), (((1,), (1,)), ((), ())), preferred_element_type=jnp.float32
        ).astype(jnp.bfloat16)

    part = [product(halves)]
    for bits, pieces in ((1, near), (2, far), (3, cross)):
        part.append(lax.ppermute(product(pieces), "seq", flip[bits]))
    place = lax.axis_index("seq")
    odd = lax.rem(place, 2) == 1
    upper = lax.rem(place, 4) >= 2
    same = [jnp.where(odd, part[1], part[0]), jnp.where(odd, part[0], part[1])]
    away = [jnp.where(odd, part[3], part[2]), jnp.where(odd, part[2], part[3])]
    ordered = [jnp.where(upper, f, e) for e, f in zip(same, away)] + [jnp.where(upper, e, f) for e, f in zip(same, away)]
    columns = jnp.concatenate([piece.reshape(count // 4, local, rows) for piece in ordered], 1)
    return columns.reshape(count * local, rows).T


def moe_kernel(
    devices, locals_, parts, tab_ref, win_ref, wdown_ref, ret_ref,
    arrive, part, wi, wd, acc, spread, act, wi_sem, wd_sem, send_sem, recv_sem, back_send, back_recv,
):
    me = lax.axis_index("seq")
    per, width = tab_ref.shape[1], tab_ref.shape[2]
    step = width // parts
    rows = devices * per
    each = rows // locals_
    blocks = win_ref.shape[1]
    mine = blocks // locals_
    hidden = mine * HEAD
    slots = per // locals_

    def columns(c):
        return pl.ds(pl.multiple_of(c * step, step), step)

    def fetch_in(c, j):
        where = pl.ds(pl.multiple_of(c * step, step), step)
        return pltpu.make_async_copy(win_ref.at[where, j], wi.at[j, where], wi_sem.at[c])

    def all_in(c):
        where = pl.ds(pl.multiple_of(c * step, step), step)
        return pltpu.make_async_copy(wi.at[:, where], wi.at[:, where], wi_sem.at[c])

    fetch_down = pltpu.make_async_copy(wdown_ref, wd, wd_sem)

    barrier = pltpu.get_barrier_semaphore()

    def greet(k, _):
        pl.semaphore_signal(barrier, inc=1, device_id=(lax.rem(me + k, devices),), device_id_type=MESH)
        return 0

    lax.fori_loop(1, devices, greet, 0)
    for c in range(parts):
        lax.fori_loop(0, blocks, lambda j, _: (fetch_in(c, j).start(), 0)[1], 0)
    fetch_down.start()
    pl.semaphore_wait(barrier, devices - 1)

    def dispatch(c):
        def send(k, _):
            peer = lax.rem(me + k, devices)
            pltpu.make_async_remote_copy(
                src_ref=tab_ref.at[peer, :, columns(c)],
                dst_ref=arrive.at[me, :, columns(c)],
                send_sem=send_sem.at[c],
                recv_sem=recv_sem.at[c],
                device_id=(peer,),
                device_id_type=MESH,
            ).start()
            return 0

        lax.fori_loop(1, devices, send, 0)
        pltpu.make_async_copy(tab_ref.at[me, :, columns(c)], arrive.at[me, :, columns(c)], recv_sem.at[c]).start()

    for c in range(parts):
        dispatch(c)

    to = lax.broadcasted_iota(jnp.int32, (rows, rows), 0)
    frm = lax.broadcasted_iota(jnp.int32, (rows, rows), 1)
    group, inner = to // each, to % each
    sort = (frm == (inner // slots) * per + group * slots + inner % slots).astype(jnp.bfloat16)
    source, place = to // per, to % per
    unsort = (frm == (place // slots) * each + source * slots + place % slots).astype(jnp.bfloat16)
    wide = lax.broadcasted_iota(jnp.int32, (HEAD, 2 * HEAD), 1)
    double = (wide // 2 == lax.broadcasted_iota(jnp.int32, (HEAD, 2 * HEAD), 0)).astype(jnp.bfloat16)
    even = lax.broadcasted_iota(jnp.int32, (rows, 2 * HEAD), 1) % 2 == 0

    for c in range(parts):
        cols = slice(c * step, (c + 1) * step)
        pltpu.make_async_copy(arrive.at[:, :, cols], arrive.at[:, :, cols], recv_sem.at[c]).wait()
        got = arrive[:, :, cols].reshape(rows, step)
        got = jnp.dot(sort, got, preferred_element_type=jnp.float32).astype(jnp.bfloat16)
        for t in range(step // HEAD):
            pair = jnp.dot(got[:, t * HEAD : (t + 1) * HEAD], double, preferred_element_type=jnp.float32)
            gate_side = jnp.where(even, pair, 0.0).astype(jnp.bfloat16)
            up_side = jnp.where(even, 0.0, pair).astype(jnp.bfloat16)
            for e in range(locals_):
                lanes = slice(2 * t * HEAD, 2 * (t + 1) * HEAD)
                spread[e, 0:each, lanes] = gate_side[e * each : (e + 1) * each]
                spread[e, each : 2 * each, lanes] = up_side[e * each : (e + 1) * each]
        all_in(c).wait()
        for e in range(locals_):
            left = spread[e]

            def weight(j):
                return wi[e * mine + j, cols].reshape(2 * step, HEAD)

            def two(p, _):
                right = jnp.concatenate([weight(2 * p), weight(2 * p + 1)], 1)
                value = jnp.dot(left, right, preferred_element_type=jnp.float32)
                acc[e, p] = value if c == 0 else acc[e, p] + value
                return 0

            lax.fori_loop(0, mine // 2, two, 0, unroll=2)
            if mine % 2:
                value = jnp.dot(left, weight(mine - 1), preferred_element_type=jnp.float32)
                last = mine // 2
                acc[e, last, :, 0:HEAD] = value if c == 0 else acc[e, last, :, 0:HEAD] + value

    for e in range(locals_):
        for p in range((mine + 1) // 2):
            size = min(2 * HEAD, hidden - 2 * HEAD * p)
            gate, up = acc[e, p, 0:each, 0:size], acc[e, p, each : 2 * each, 0:size]
            act[e, :, 2 * HEAD * p : 2 * HEAD * p + size] = (jax.nn.silu(gate) * up).astype(jnp.bfloat16)

    fetch_down.wait()

    def finish(c, _):
        cols = columns(c)
        pieces = []
        for e in range(locals_):
            pieces.append(
                jnp.dot(
                    act[e], wd[e * hidden : (e + 1) * hidden, cols], preferred_element_type=jnp.float32
                ).astype(jnp.bfloat16)
            )
        out = jnp.dot(unsort, jnp.concatenate(pieces, 0), preferred_element_type=jnp.float32)
        part[:, :, cols] = out.astype(jnp.bfloat16).reshape(devices, per, step)

        def send(k, _):
            peer = lax.rem(me + k, devices)
            pltpu.make_async_remote_copy(
                src_ref=part.at[peer, :, cols],
                dst_ref=ret_ref.at[me, :, cols],
                send_sem=back_send.at[c],
                recv_sem=back_recv.at[c],
                device_id=(peer,),
                device_id_type=MESH,
            ).start()
            return 0

        lax.fori_loop(1, devices, send, 0)
        pltpu.make_async_copy(part.at[me, :, cols], ret_ref.at[me, :, cols], back_recv.at[c]).start()
        return 0

    lax.fori_loop(0, parts, finish, 0)
    for c in range(parts):
        cols = slice(c * step, (c + 1) * step)
        others = slice(0, devices - 1)
        pltpu.make_async_copy(tab_ref.at[others, :, cols], arrive.at[others, :, cols], send_sem.at[c]).wait()
        pltpu.make_async_copy(part.at[others, :, cols], arrive.at[others, :, cols], back_send.at[c]).wait()
        pltpu.make_async_copy(ret_ref.at[:, :, cols], ret_ref.at[:, :, cols], back_recv.at[c]).wait()


def moe(table, expert_in, expert_down, locals_, parts):
    devices, per, width = table.shape
    blocks = expert_in.shape[2] // HEAD
    mine = blocks // locals_
    step = width // parts
    each = devices * per // locals_
    view = expert_in.reshape(width, 2, blocks, HEAD).transpose(0, 2, 1, 3)
    shape = (devices, per, width)
    return pl.pallas_call(
        functools.partial(moe_kernel, devices, locals_, parts),
        out_shape=jax.ShapeDtypeStruct(shape, jnp.bfloat16),
        in_specs=[
            pl.BlockSpec(memory_space=pltpu.VMEM),
            pl.BlockSpec(memory_space=pl.ANY),
            pl.BlockSpec(memory_space=pl.ANY),
        ],
        out_specs=pl.BlockSpec(memory_space=pltpu.VMEM),
        scratch_shapes=[
            pltpu.VMEM(shape, jnp.bfloat16),
            pltpu.VMEM(shape, jnp.bfloat16),
            pltpu.VMEM((blocks, width, 2, HEAD), jnp.bfloat16),
            pltpu.VMEM(expert_down.shape, jnp.bfloat16),
            pltpu.VMEM((locals_, (mine + 1) // 2, 2 * each, 2 * HEAD), jnp.float32),
            pltpu.VMEM((locals_, 2 * each, 2 * step), jnp.bfloat16),
            pltpu.VMEM((locals_, each, mine * HEAD), jnp.bfloat16),
            pltpu.SemaphoreType.DMA((parts,)),
            pltpu.SemaphoreType.DMA,
            pltpu.SemaphoreType.DMA((parts,)),
            pltpu.SemaphoreType.DMA((parts,)),
            pltpu.SemaphoreType.DMA((parts,)),
            pltpu.SemaphoreType.DMA((parts,)),
        ],
        compiler_params=pltpu.CompilerParams(
            collective_id=0, has_side_effects=True, vmem_limit_bytes=66 * 1024 * 1024 - 2**21
        ),
        cost_estimate=pl.CostEstimate(flops=10**10, bytes_accessed=51 << 20, transcendentals=0),
        name="moe",
    )(table, view, expert_down)


def body(
    residual,
    queries,
    keys,
    values,
    out_proj,
    norm_gain,
    expert_in,
    expert_down,
    routes,
    gate_ints,
    modality,
    capacity,
):
    devices = lax.axis_size("seq")
    tok_rows = residual.shape[0]
    width_d = residual.shape[1]
    chips_back = ((WINDOW + tok_rows - 1) // tok_rows + 1) // 2
    mine, other = window_blocks(jnp.concatenate([keys, values], 1), chips_back)
    local_experts = max(1, EXPERTS // devices)
    hidden_each = expert_in.shape[2] // local_experts
    mine, other = lax.optimization_barrier((mine, other))
    halves = [attend(queries, mine, other, chips_back, part) for part in range(2)]
    attended = project(halves, out_proj)
    attended = lax.optimization_barrier(attended)
    hidden = residual.astype(jnp.float32) + attended.astype(jnp.float32)
    normed = (
        hidden * lax.rsqrt(jnp.mean(hidden * hidden, -1, keepdims=True) + 1e-05) * norm_gain
    ).astype(jnp.bfloat16)
    slot_count = 2 * CAP
    split_ways = max(1, devices // EXPERTS)
    chosen = routes.reshape(-1)
    modal_flag = jnp.repeat(modality, 2)
    slot_key = chosen * 2 + modal_flag
    choices = slot_key.shape[0]
    order = jnp.arange(choices, dtype=jnp.int32)
    rank_in = jnp.sum(
        ((slot_key[:, None] == slot_key[None, :]) & (order[None, :] < order[:, None])).astype(jnp.int32), 1
    )
    onehot = slot_key[:, None] == jnp.arange(2 * EXPERTS, dtype=jnp.int32)[None, :]
    limit_of = jnp.sum(jnp.where(onehot, capacity.reshape(1, -1), 0), 1)
    kept_mask = rank_in < limit_of
    column = chosen * slot_count + modal_flag * CAP + rank_in
    column = jnp.where(kept_mask, column, -1).reshape(tok_rows, 2)
    holders = EXPERTS // local_experts
    high = (gate_ints & ~7).astype(jnp.float32) / 1024.0
    low = (gate_ints & 7).astype(jnp.float32) / 1024.0
    per = local_experts * slot_count
    if split_ways == 1 and per % 8 == 0 and hidden_each % HEAD == 0 and width_d % (4 * HEAD) == 0:
        ids = jnp.arange(EXPERTS * slot_count, dtype=jnp.int32)
        hit = column[:, :, None] == ids[None, None, :]
        select = jnp.any(hit, 1).astype(jnp.bfloat16)
        comb_high = jnp.sum(jnp.where(hit, high[:, :, None], 0.0), 1).astype(jnp.bfloat16)
        comb_low = jnp.sum(jnp.where(hit, low[:, :, None], 0.0), 1).astype(jnp.bfloat16)
        table = lax.dot_general(
            select, normed, (((0,), (0,)), ((), ())), preferred_element_type=jnp.float32
        ).astype(jnp.bfloat16)
        back = moe(table.reshape(devices, per, width_d), expert_in, expert_down, local_experts, 4)
        both = jnp.dot(
            jnp.concatenate([comb_high, comb_low], 0),
            back.reshape(devices * per, width_d),
            preferred_element_type=jnp.float32,
        )
        return (attended, (both[:tok_rows] + both[tok_rows:]).astype(jnp.bfloat16))
    slot_ids = jnp.arange(EXPERTS * slot_count, dtype=jnp.int32).reshape(holders, local_experts, slot_count)
    total = jnp.zeros((tok_rows, width_d), jnp.float32)
    for local in range(local_experts):
        ids = slot_ids[:, local].reshape(-1)
        hit = column[:, :, None] == ids[None, None, :]
        select = jnp.any(hit, 1).astype(jnp.bfloat16)
        comb_high = jnp.sum(jnp.where(hit, high[:, :, None], 0.0), 1).astype(jnp.bfloat16)
        comb_low = jnp.sum(jnp.where(hit, low[:, :, None], 0.0), 1).astype(jnp.bfloat16)
        table = lax.dot_general(
            select, normed, (((0,), (0,)), ((), ())), preferred_element_type=jnp.float32
        ).astype(jnp.bfloat16)
        outgoing = jnp.repeat(table.reshape(holders, slot_count, width_d), split_ways, 0)
        arrived = lax.all_to_all(outgoing, "seq", split_axis=0, concat_axis=0, tiled=True)
        rows_in = arrived.reshape(devices * slot_count, width_d)
        first = local * hidden_each
        gate_up = jnp.einsum(
            "kd,dgf->gkf", rows_in, expert_in[:, :, first : first + hidden_each], preferred_element_type=jnp.float32
        )
        active = (jax.nn.silu(gate_up[0]) * gate_up[1]).astype(jnp.bfloat16)
        part = jnp.dot(
            active, expert_down[first : first + hidden_each], preferred_element_type=jnp.float32
        ).astype(jnp.bfloat16)
        returned = lax.all_to_all(
            part.reshape(devices, slot_count, width_d), "seq", split_axis=0, concat_axis=0, tiled=True
        )
        if split_ways > 1:
            returned = jnp.sum(
                returned.reshape(holders, split_ways, slot_count, width_d).astype(jnp.float32), 1
            ).astype(jnp.bfloat16)
        mixed = returned.reshape(holders * slot_count, width_d)
        total = (
            total
            + jnp.dot(comb_high, mixed, preferred_element_type=jnp.float32)
            + jnp.dot(comb_low, mixed, preferred_element_type=jnp.float32)
        )
    return (attended, total.astype(jnp.bfloat16))


def solution(mesh):
    placed = (
        P("seq", None),
        P("seq", None),
        P("seq", None),
        P("seq", None),
        P(None, "seq"),
        P(),
        P(None, None, "seq"),
        P("seq", None),
        P("seq", None),
        P("seq", None),
        P("seq"),
        P(),
    )
    return jax.shard_map(
        body,
        mesh=mesh,
        in_specs=placed,
        out_specs=(P("seq", None), P("seq", None)),
        check_vma=False,
    )
```

```python
import functools
import math
import jax
import jax.numpy as jnp
from jax import lax
from jax.experimental import pallas as pl
from jax.experimental.pallas import tpu as pltpu
from jax.sharding import PartitionSpec as P

HEADS = 20
KV_HEADS = 4
HEAD = 128
WINDOW = 1024
EXPERTS = 64
CAP = 2
MESH = pl.DeviceIdType.MESH


def window_blocks(own, chips_back):
    count = lax.axis_size("seq")
    swap = [(source, source ^ 1) for source in range(count)]
    span = 2 * chips_back
    mine = {0: own}
    prev = lax.ppermute(own, "seq", [(s, s + span) for s in range(count - span)])
    mine[chips_back] = prev
    if count % span == 0:
        place = lax.rem(lax.axis_index("seq"), span) // 2
        for step in range(1, chips_back):
            payload = jnp.where(place + step < chips_back, own, prev)
            turn = [(s, s - s % span + (s % span + 2 * step) % span) for s in range(count)]
            mine[step] = lax.ppermute(payload, "seq", turn)
    else:
        for step in range(1, chips_back):
            mine[step] = lax.ppermute(own, "seq", [(s, s + 2 * step) for s in range(count - 2 * step)])
    other = {step: lax.ppermute(block, "seq", swap) for step, block in mine.items()}
    return mine, other


def attend_kernel(chips_back, rows, q_ref, *refs):
    out_ref = refs[-1]
    blocks = 2 * (chips_back + 1)
    k_refs, v_refs = refs[:blocks], refs[blocks : 2 * blocks]
    me = lax.axis_index("seq")
    core = lax.rem(me, 2)
    keys = jnp.concatenate([ref[...] for ref in k_refs], 0)
    vals = jnp.concatenate([ref[...] for ref in v_refs], 0)
    q_pos = me * rows + lax.broadcasted_iota(jnp.int32, (rows, rows), 0)
    lane = lax.broadcasted_iota(jnp.int32, (rows, rows), 1)
    bias = []
    for half in range(2):
        for step in range(chips_back + 1):
            block = (me - core) - 2 * step + (core if half == 0 else 1 - core)
            k_pos = block * rows + lane
            seen = (k_pos <= q_pos) & (k_pos > q_pos - WINDOW) & (k_pos >= 0)
            bias.append(jnp.where(seen, 0.0, -1e30))
    bias = jnp.concatenate(bias, 1)
    scale = HEAD ** (-0.5) * math.log2(math.e)
    for g in range(HEADS // KV_HEADS):
        q_one = q_ref[:, g * HEAD : (g + 1) * HEAD]
        scores = lax.dot_general(q_one, keys, (((1,), (1,)), ((), ())), preferred_element_type=jnp.float32)
        scores = scores * scale + bias
        weights = jnp.exp2(scores - jnp.max(scores, -1, keepdims=True))
        total = jnp.sum(weights, -1, keepdims=True)
        probs = (weights * (1.0 / total)).astype(jnp.bfloat16)
        mixed = jnp.dot(probs, vals, preferred_element_type=jnp.float32)
        out_ref[:, g * HEAD : (g + 1) * HEAD] = mixed.astype(jnp.bfloat16)


def attend(queries, mine, other, chips_back, part):
    rows = queries.shape[0]
    wide = HEADS // KV_HEADS * HEAD
    ordered = [mine[s] for s in range(chips_back + 1)] + [other[s] for s in range(chips_back + 1)]
    heads = KV_HEADS // 2
    first = part * heads
    k_spec = pl.BlockSpec((rows, HEAD), lambda h: (0, first + h))
    v_spec = pl.BlockSpec((rows, HEAD), lambda h: (0, KV_HEADS + first + h))
    q_spec = pl.BlockSpec((rows, wide), lambda h: (0, first + h))
    span = rows * len(ordered)
    return pl.pallas_call(
        functools.partial(attend_kernel, chips_back, rows),
        grid=(heads,),
        out_shape=jax.ShapeDtypeStruct((rows, heads * wide), jnp.bfloat16),
        in_specs=[q_spec] + [k_spec] * len(ordered) + [v_spec] * len(ordered),
        out_specs=pl.BlockSpec((rows, wide), lambda h: (0, h)),
        cost_estimate=pl.CostEstimate(
            flops=2 * HEADS * rows * span * HEAD, bytes_accessed=4 << 20, transcendentals=HEADS * rows * span // 2
        ),
        name="attend",
    )(queries, *ordered, *ordered)


def project(halves, out_proj):
    count = lax.axis_size("seq")
    flip = [[(source, source ^ bits) for source in range(count)] for bits in range(4)]
    classes = [[s for s in range(count) if s % 4 == kind] for kind in range(4)]
    weights = lax.all_gather(out_proj.T, "seq", axis=0, tiled=True, axis_index_groups=classes)
    far = [lax.ppermute(half, "seq", flip[2]) for half in halves]
    near = [lax.ppermute(half, "seq", flip[1]) for half in halves]
    cross = [lax.ppermute(half, "seq", flip[1]) for half in far]
    return gather_columns(weights, [jnp.concatenate(pieces, 1) for pieces in (halves, near, far, cross)])


def gather_columns(weights, contexts):
    count = lax.axis_size("seq")
    rows = contexts[0].shape[0]
    local = weights.shape[0] * 4 // count
    flip = [[(source, source ^ bits) for source in range(count)] for bits in range(4)]

    def product(context):
        return lax.dot_general(
            weights, context, (((1,), (1,)), ((), ())), preferred_element_type=jnp.float32
        ).astype(jnp.bfloat16)

    part = [None] * 4
    for bits in (2, 3, 1):
        part[bits] = lax.ppermute(product(contexts[bits]), "seq", flip[bits])
    part[0] = product(contexts[0])
    place = lax.axis_index("seq")
    odd = lax.rem(place, 2) == 1
    upper = lax.rem(place, 4) >= 2
    same = [jnp.where(odd, part[1], part[0]), jnp.where(odd, part[0], part[1])]
    away = [jnp.where(odd, part[3], part[2]), jnp.where(odd, part[2], part[3])]
    ordered = [jnp.where(upper, f, e) for e, f in zip(same, away)] + [jnp.where(upper, e, f) for e, f in zip(same, away)]
    columns = jnp.concatenate([piece.reshape(count // 4, local, rows) for piece in ordered], 1)
    return columns.reshape(count * local, rows).T


def moe_kernel(
    devices, locals_, parts, tab_ref, win_ref, wdown_ref, ret_ref,
    arrive, part, wi, wd, acc, spread, act, wi_sem, wd_sem, send_sem, recv_sem, back_send, back_recv,
):
    me = lax.axis_index("seq")
    per, width = tab_ref.shape[1], tab_ref.shape[2]
    step = width // parts
    rows = devices * per
    each = rows // locals_
    blocks = win_ref.shape[1]
    mine = blocks // locals_
    hidden = mine * HEAD
    slots = per // locals_

    def columns(c):
        return pl.ds(pl.multiple_of(c * step, step), step)

    def fetch_in(c, j):
        where = pl.ds(pl.multiple_of(c * step, step), step)
        return pltpu.make_async_copy(win_ref.at[where, j], wi.at[j, where], wi_sem.at[c])

    def all_in(c):
        where = pl.ds(pl.multiple_of(c * step, step), step)
        return pltpu.make_async_copy(wi.at[:, where], wi.at[:, where], wi_sem.at[c])

    fetch_down = pltpu.make_async_copy(wdown_ref, wd, wd_sem)

    barrier = pltpu.get_barrier_semaphore()

    def greet(k, _):
        pl.semaphore_signal(barrier, inc=1, device_id=(lax.rem(me + k, devices),), device_id_type=MESH)
        return 0

    lax.fori_loop(1, devices, greet, 0)
    for c in range(parts):
        lax.fori_loop(0, blocks, lambda j, _: (fetch_in(c, j).start(), 0)[1], 0)
    fetch_down.start()
    pl.semaphore_wait(barrier, devices - 1)

    def dispatch(c):
        def send(k, _):
            peer = lax.rem(me + k, devices)
            pltpu.make_async_remote_copy(
                src_ref=tab_ref.at[peer, :, columns(c)],
                dst_ref=arrive.at[me, :, columns(c)],
                send_sem=send_sem.at[c],
                recv_sem=recv_sem.at[c],
                device_id=(peer,),
                device_id_type=MESH,
            ).start()
            return 0

        lax.fori_loop(1, devices, send, 0)
        pltpu.make_async_copy(tab_ref.at[me, :, columns(c)], arrive.at[me, :, columns(c)], recv_sem.at[c]).start()

    for c in range(parts):
        dispatch(c)

    to = lax.broadcasted_iota(jnp.int32, (rows, rows), 0)
    frm = lax.broadcasted_iota(jnp.int32, (rows, rows), 1)
    group, inner = to // each, to % each
    sort = (frm == (inner // slots) * per + group * slots + inner % slots).astype(jnp.bfloat16)
    source, place = to // per, to % per
    unsort = (frm == (place // slots) * each + source * slots + place % slots).astype(jnp.bfloat16)
    wide = lax.broadcasted_iota(jnp.int32, (HEAD, 2 * HEAD), 1)
    double = (wide // 2 == lax.broadcasted_iota(jnp.int32, (HEAD, 2 * HEAD), 0)).astype(jnp.bfloat16)
    even = lax.broadcasted_iota(jnp.int32, (rows, 2 * HEAD), 1) % 2 == 0

    for c in range(parts):
        cols = slice(c * step, (c + 1) * step)
        pltpu.make_async_copy(arrive.at[:, :, cols], arrive.at[:, :, cols], recv_sem.at[c]).wait()
        got = arrive[:, :, cols].reshape(rows, step)
        got = jnp.dot(sort, got, preferred_element_type=jnp.float32).astype(jnp.bfloat16)
        for t in range(step // HEAD):
            pair = jnp.dot(got[:, t * HEAD : (t + 1) * HEAD], double, preferred_element_type=jnp.float32)
            gate_side = jnp.where(even, pair, 0.0).astype(jnp.bfloat16)
            up_side = jnp.where(even, 0.0, pair).astype(jnp.bfloat16)
            for e in range(locals_):
                lanes = slice(2 * t * HEAD, 2 * (t + 1) * HEAD)
                spread[e, 0:each, lanes] = gate_side[e * each : (e + 1) * each]
                spread[e, each : 2 * each, lanes] = up_side[e * each : (e + 1) * each]
        all_in(c).wait()
        for e in range(locals_):
            left = spread[e]

            def weight(j):
                return wi[e * mine + j, cols].reshape(2 * step, HEAD)

            def two(p, _):
                right = jnp.concatenate([weight(2 * p), weight(2 * p + 1)], 1)
                value = jnp.dot(left, right, preferred_element_type=jnp.float32)
                acc[e, p] = value if c == 0 else acc[e, p] + value
                return 0

            lax.fori_loop(0, mine // 2, two, 0, unroll=2)
            if mine % 2:
                value = jnp.dot(left, weight(mine - 1), preferred_element_type=jnp.float32)
                last = mine // 2
                acc[e, last, :, 0:HEAD] = value if c == 0 else acc[e, last, :, 0:HEAD] + value

    for e in range(locals_):
        for p in range((mine + 1) // 2):
            size = min(2 * HEAD, hidden - 2 * HEAD * p)
            gate, up = acc[e, p, 0:each, 0:size], acc[e, p, each : 2 * each, 0:size]
            act[e, :, 2 * HEAD * p : 2 * HEAD * p + size] = (jax.nn.silu(gate) * up).astype(jnp.bfloat16)

    fetch_down.wait()

    def finish(c, _):
        cols = columns(c)
        pieces = []
        for e in range(locals_):
            pieces.append(
                jnp.dot(
                    act[e], wd[e * hidden : (e + 1) * hidden, cols], preferred_element_type=jnp.float32
                ).astype(jnp.bfloat16)
            )
        out = jnp.dot(unsort, jnp.concatenate(pieces, 0), preferred_element_type=jnp.float32)
        part[:, :, cols] = out.astype(jnp.bfloat16).reshape(devices, per, step)

        def send(k, _):
            peer = lax.rem(me + k, devices)
            pltpu.make_async_remote_copy(
                src_ref=part.at[peer, :, cols],
                dst_ref=ret_ref.at[me, :, cols],
                send_sem=back_send.at[c],
                recv_sem=back_recv.at[c],
                device_id=(peer,),
                device_id_type=MESH,
            ).start()
            return 0

        lax.fori_loop(1, devices, send, 0)
        pltpu.make_async_copy(part.at[me, :, cols], ret_ref.at[me, :, cols], back_recv.at[c]).start()
        return 0

    lax.fori_loop(0, parts, finish, 0)
    for c in range(parts):
        cols = slice(c * step, (c + 1) * step)
        others = slice(0, devices - 1)
        pltpu.make_async_copy(tab_ref.at[others, :, cols], arrive.at[others, :, cols], send_sem.at[c]).wait()
        pltpu.make_async_copy(part.at[others, :, cols], arrive.at[others, :, cols], back_send.at[c]).wait()
        pltpu.make_async_copy(ret_ref.at[:, :, cols], ret_ref.at[:, :, cols], back_recv.at[c]).wait()


def moe(table, expert_in, expert_down, locals_, parts):
    devices, per, width = table.shape
    blocks = expert_in.shape[2] // HEAD
    mine = blocks // locals_
    step = width // parts
    each = devices * per // locals_
    view = expert_in.reshape(width, 2, blocks, HEAD).transpose(0, 2, 1, 3)
    shape = (devices, per, width)
    return pl.pallas_call(
        functools.partial(moe_kernel, devices, locals_, parts),
        out_shape=jax.ShapeDtypeStruct(shape, jnp.bfloat16),
        in_specs=[
            pl.BlockSpec(memory_space=pltpu.VMEM),
            pl.BlockSpec(memory_space=pl.ANY),
            pl.BlockSpec(memory_space=pl.ANY),
        ],
        out_specs=pl.BlockSpec(memory_space=pltpu.VMEM),
        scratch_shapes=[
            pltpu.VMEM(shape, jnp.bfloat16),
            pltpu.VMEM(shape, jnp.bfloat16),
            pltpu.VMEM((blocks, width, 2, HEAD), jnp.bfloat16),
            pltpu.VMEM(expert_down.shape, jnp.bfloat16),
            pltpu.VMEM((locals_, (mine + 1) // 2, 2 * each, 2 * HEAD), jnp.float32),
            pltpu.VMEM((locals_, 2 * each, 2 * step), jnp.bfloat16),
            pltpu.VMEM((locals_, each, mine * HEAD), jnp.bfloat16),
            pltpu.SemaphoreType.DMA((parts,)),
            pltpu.SemaphoreType.DMA,
            pltpu.SemaphoreType.DMA((parts,)),
            pltpu.SemaphoreType.DMA((parts,)),
            pltpu.SemaphoreType.DMA((parts,)),
            pltpu.SemaphoreType.DMA((parts,)),
        ],
        compiler_params=pltpu.CompilerParams(
            collective_id=0, has_side_effects=True, vmem_limit_bytes=66 * 1024 * 1024 - 2**21
        ),
        cost_estimate=pl.CostEstimate(flops=10**10, bytes_accessed=51 << 20, transcendentals=0),
        name="moe",
    )(table, view, expert_down)


def front_kernel(
    cut, q_any, k_ref, v_ref, w_ref, ctx_ref, wg_ref,
    q_ref, km, vm, ko, vo, bias_ref,
    q_sem, kv_send, mine_sem, other_sem, up_send, down_send, side_send, whole_sem, tail_sem, own_sem, ctx_send, ctx_recv,
):
    count = lax.axis_size("seq")
    me = lax.axis_index("seq")
    rows = q_any.shape[0]
    near_steps = km.shape[0] - 1
    span = 2 * near_steps
    planes = count // span
    local = w_ref.shape[0]
    plane = me // span
    inside = me % span
    place = inside // 2
    core = me % 2
    column = inside // 4
    pal = me + 1 - 2 * core
    across = me + 2 - 4 * (place % 2)
    side = me + 4 - 8 * column
    above, below = me + span, me - span
    has_above, has_below = plane + 1 < planes, plane >= 1

    def remote(src, dst, send, recv, peer):
        return pltpu.make_async_remote_copy(
            src_ref=src, dst_ref=dst, send_sem=send, recv_sem=recv, device_id=(peer,), device_id_type=MESH
        )

    def landed(ref, sem):
        pltpu.make_async_copy(ref, ref, sem).wait()

    load = pltpu.make_async_copy(q_any, q_ref, q_sem)
    load.start()
    barrier = pltpu.get_barrier_semaphore()

    def greet(peer):
        pl.semaphore_signal(barrier, inc=1, device_id=(peer,), device_id_type=MESH)

    def turned(step):
        return me - inside + (inside + 2 * step) % span

    greet(pal)
    for step in range(1, near_steps):
        greet(turned(step))
    pl.when(has_above)(lambda: greet(above))
    pl.when(has_below)(lambda: greet(below))
    pl.semaphore_wait(
        barrier, near_steps + has_above.astype(jnp.int32) + has_below.astype(jnp.int32)
    )

    def kv(src_k, src_v, dst_k, dst_v, lane, recv, peer):
        return [
            remote(src_k, dst_k, kv_send.at[lane, 0], recv.at[0], peer),
            remote(src_v, dst_v, kv_send.at[lane, 1], recv.at[1], peer),
        ]

    def go(copies):
        for copy in copies:
            copy.start()

    def rise():
        return kv(k_ref, v_ref, km.at[near_steps], vm.at[near_steps], 0, mine_sem.at[near_steps], above)

    def turn(step, late):
        a, b = (km.at[near_steps], vm.at[near_steps]) if late else (k_ref, v_ref)
        return kv(a, b, km.at[step], vm.at[step], step, mine_sem.at[step], turned(step))

    def share(step):
        a, b = (km.at[step], vm.at[step]) if step else (k_ref, v_ref)
        return kv(a, b, ko.at[step], vo.at[step], near_steps + step, other_sem.at[step], pal)

    def early(step):
        return (place + step < near_steps) | (plane == 0)

    pl.when(has_above)(lambda: go(rise()))
    for step in range(1, near_steps):
        pl.when(early(step))(lambda step=step: go(turn(step, False)))
    go(share(0))
    go([
        pltpu.make_async_copy(k_ref, km.at[0], mine_sem.at[0, 0]),
        pltpu.make_async_copy(v_ref, vm.at[0], mine_sem.at[0, 1]),
    ])

    @pl.when(plane == 0)
    def _():
        go([
            pltpu.make_async_copy(k_ref, km.at[near_steps], mine_sem.at[near_steps, 0]),
            pltpu.make_async_copy(v_ref, vm.at[near_steps], mine_sem.at[near_steps, 1]),
        ])

    head, tail = pl.ds(0, cut), pl.ds(cut, local - cut)

    def slot(level, col):
        return 2 * level + col

    def lift(hop, upward):
        level = plane - hop if upward else plane + hop
        peer = above if upward else below
        sends = up_send if upward else down_send
        s = slot(level, column)
        src = w_ref if hop == 0 else wg_ref.at[s]
        return remote(src, wg_ref.at[s], sends.at[hop, 0], whole_sem.at[s], peer)

    def lift_tail(hop, upward):
        level = plane - hop if upward else plane + hop
        peer = above if upward else below
        sends = up_send if upward else down_send
        s = slot(level, 1 - column)
        return remote(wg_ref.at[s, tail], wg_ref.at[s, tail], sends.at[hop, 1], tail_sem.at[s], peer)

    def across_side(hop, upward):
        level = plane - hop if upward else plane + hop
        s = slot(level, column)
        src = w_ref.at[head] if hop == 0 else wg_ref.at[s, head]
        return remote(src, wg_ref.at[s, head], side_send.at[level], whole_sem.at[s], side)

    def side_tail():
        s = slot(plane, column)
        return remote(w_ref.at[tail], wg_ref.at[s, tail], side_send.at[planes], tail_sem.at[s], side)

    side_tail().start()
    pl.when(has_above)(lambda: lift(0, True).start())
    pl.when(has_below)(lambda: lift(0, False).start())
    across_side(0, True).start()
    own_slot = slot(plane, column)
    keep = pltpu.make_async_copy(w_ref, wg_ref.at[own_slot], own_sem)
    keep.start()

    def first_tail():
        s = slot(plane, 1 - column)
        landed(wg_ref.at[s, tail], tail_sem.at[s])
        pl.when(has_above)(lambda: lift_tail(0, True).start())
        pl.when(has_below)(lambda: lift_tail(0, False).start())

    def relay(hop):
        for upward in (True, False):
            level = plane - hop if upward else plane + hop
            here = level >= 0 if upward else level < planes
            more = has_above if upward else has_below

            @pl.when(here)
            def _():
                s = slot(level, column)
                landed(wg_ref.at[s], whole_sem.at[s])
                pl.when(more)(lambda: lift(hop, upward).start())
                across_side(hop, upward).start()
                o = slot(level, 1 - column)
                landed(wg_ref.at[o, tail], tail_sem.at[o])
                pl.when(more)(lambda: lift_tail(hop, upward).start())

    def mine_landed(step):
        landed(km.at[step], mine_sem.at[step, 0])
        landed(vm.at[step], mine_sem.at[step, 1])

    q_pos = me * rows + lax.broadcasted_iota(jnp.int32, (rows, rows), 0)
    lane = lax.broadcasted_iota(jnp.int32, (rows, rows), 1)
    for half in range(2):
        for step in range(near_steps + 1):
            block = (me - core) - 2 * step + (core if half == 0 else 1 - core)
            k_pos = block * rows + lane
            seen = (k_pos <= q_pos) & (k_pos > q_pos - WINDOW) & (k_pos >= 0)
            at = (half * (near_steps + 1) + step) * rows
            bias_ref[:, at : at + rows] = jnp.where(seen, 0.0, -1e30)

    mine_landed(near_steps)
    for step in range(1, near_steps):
        pl.when(jnp.logical_not(early(step)))(lambda step=step: go(turn(step, True)))
    go(share(near_steps))
    first_tail()
    mine_landed(0)
    for step in range(1, near_steps):
        mine_landed(step)
        go(share(step))
    relay(1)
    for step in range(near_steps + 1):
        landed(ko.at[step], other_sem.at[step, 0])
        landed(vo.at[step], other_sem.at[step, 1])

    load.wait()
    scale = HEAD ** (-0.5) * math.log2(math.e)
    heads = HEADS // KV_HEADS
    wide = heads * HEAD

    def context(g, peer_kind):
        cols = pl.ds(pl.multiple_of(g * wide, wide), wide)
        peer = pal if peer_kind == 0 else across
        return remote(
            ctx_ref.at[0, :, cols], ctx_ref.at[1 + peer_kind, :, cols],
            ctx_send.at[peer_kind, g], ctx_recv.at[peer_kind, g], peer,
        )

    def passed(g):
        cols = pl.ds(pl.multiple_of(g * wide, wide), wide)
        return remote(ctx_ref.at[2, :, cols], ctx_ref.at[3, :, cols], ctx_send.at[2, g], ctx_recv.at[2, g], pal)

    def group(g, _):
        cols = pl.ds(pl.multiple_of(g * HEAD, HEAD), HEAD)
        keys = jnp.concatenate(
            [ref[s, :, cols] for ref in (km, ko) for s in range(near_steps + 1)], 0
        )
        vals = jnp.concatenate(
            [ref[s, :, cols] for ref in (vm, vo) for s in range(near_steps + 1)], 0
        )
        for h in range(heads):
            at = pl.ds(pl.multiple_of(g * wide + h * HEAD, HEAD), HEAD)
            scores = lax.dot_general(
                q_ref[:, at], keys, (((1,), (1,)), ((), ())), preferred_element_type=jnp.float32
            )
            scores = scores * scale + bias_ref[...]
            weights = jnp.exp2(scores - jnp.max(scores, -1, keepdims=True))
            total = jnp.sum(weights, -1, keepdims=True)
            mixed = jnp.dot(weights.astype(jnp.bfloat16), vals, preferred_element_type=jnp.float32)
            ctx_ref[0, :, at] = (mixed * (1.0 / total)).astype(jnp.bfloat16)
        context(g, 1).start()
        context(g, 0).start()
        pl.when(g == 1)(lambda: relay(2))
        return 0

    lax.fori_loop(0, KV_HEADS, group, 0)
    for hop in range(3, planes):
        relay(hop)

    for g in range(KV_HEADS):
        cols = slice(g * wide, (g + 1) * wide)
        landed(ctx_ref.at[2, :, cols], ctx_recv.at[1, g])
        passed(g).start()
    for level in range(planes):
        s = slot(level, 1 - column)
        landed(wg_ref.at[s, head], whole_sem.at[s])
    keep.wait()
    for g in range(KV_HEADS):
        cols = slice(g * wide, (g + 1) * wide)
        landed(ctx_ref.at[1, :, cols], ctx_recv.at[0, g])
        landed(ctx_ref.at[3, :, cols], ctx_recv.at[2, g])
        context(g, 0).wait_send()
        context(g, 1).wait_send()
        passed(g).wait_send()

    def sent(copies):
        for copy in copies:
            copy.wait_send()

    pl.when(has_above)(lambda: sent(rise()))
    for step in range(1, near_steps):
        sent(turn(step, False))
    for step in range(near_steps + 1):
        sent(share(step))
    sent([side_tail(), across_side(0, True)])
    for upward in (True, False):
        more = has_above if upward else has_below
        pl.when(more)(lambda upward=upward: sent([lift(0, upward), lift_tail(0, upward)]))
        for hop in range(1, planes):
            level = plane - hop if upward else plane + hop
            here = level >= 0 if upward else level < planes
            pl.when(here)(lambda hop=hop, upward=upward: sent([across_side(hop, upward)]))
            pl.when(here & more)(
                lambda hop=hop, upward=upward: sent([lift(hop, upward), lift_tail(hop, upward)])
            )


def front(queries, keys, values, columns, near_steps):
    count = lax.axis_size("seq")
    rows, wide = queries.shape
    span = 2 * near_steps
    planes = count // span
    local = columns.shape[0]
    cut = local * 4 // 5 // 8 * 8
    narrow = keys.shape[1]
    vmem = pl.BlockSpec(memory_space=pltpu.VMEM)
    dma = pltpu.SemaphoreType.DMA
    blocks = pltpu.VMEM((near_steps + 1, rows, narrow), jnp.bfloat16)
    return pl.pallas_call(
        functools.partial(front_kernel, cut),
        out_shape=(
            jax.ShapeDtypeStruct((4, rows, wide), jnp.bfloat16),
            jax.ShapeDtypeStruct((2 * planes, local, wide), jnp.bfloat16),
        ),
        in_specs=[pl.BlockSpec(memory_space=pl.ANY)] * 4,
        out_specs=(vmem, vmem),
        scratch_shapes=[
            pltpu.VMEM((rows, wide), jnp.bfloat16),
            blocks, blocks, blocks, blocks,
            pltpu.VMEM((rows, 2 * (near_steps + 1) * rows), jnp.float32),
            dma,
            dma((2 * near_steps + 1, 2)),
            dma((near_steps + 1, 2)),
            dma((near_steps + 1, 2)),
            dma((planes, 2)),
            dma((planes, 2)),
            dma((planes + 1,)),
            dma((2 * planes,)),
            dma((2 * planes,)),
            dma,
            dma((3, KV_HEADS)),
            dma((3, KV_HEADS)),
        ],
        compiler_params=pltpu.CompilerParams(
            collective_id=1, has_side_effects=True, vmem_limit_bytes=40 * 1024 * 1024
        ),
        cost_estimate=pl.CostEstimate(flops=2 * 10**9, bytes_accessed=8 << 20, transcendentals=0),
        name="front",
    )(queries, keys, values, columns)


def body(
    residual,
    queries,
    keys,
    values,
    out_proj,
    norm_gain,
    expert_in,
    expert_down,
    routes,
    gate_ints,
    modality,
    capacity,
):
    devices = lax.axis_size("seq")
    tok_rows = residual.shape[0]
    width_d = residual.shape[1]
    chips_back = ((WINDOW + tok_rows - 1) // tok_rows + 1) // 2
    local_experts = max(1, EXPERTS // devices)
    hidden_each = expert_in.shape[2] // local_experts
    if devices % (2 * chips_back) == 0 and chips_back == 4 and out_proj.shape[1] % 16 == 0:
        contexts, gathered = front(queries, keys, values, out_proj.T, chips_back)
        weights = gathered.reshape(devices // 4 * out_proj.shape[1], width_d)
        attended = gather_columns(weights, [contexts[bits] for bits in range(4)])
    else:
        mine, other = window_blocks(jnp.concatenate([keys, values], 1), chips_back)
        halves = [attend(queries, mine, other, chips_back, part) for part in range(2)]
        attended = project(halves, out_proj)
    attended = lax.optimization_barrier(attended)
    hidden = residual.astype(jnp.float32) + attended.astype(jnp.float32)
    normed = (
        hidden * lax.rsqrt(jnp.mean(hidden * hidden, -1, keepdims=True) + 1e-05) * norm_gain
    ).astype(jnp.bfloat16)
    slot_count = 2 * CAP
    split_ways = max(1, devices // EXPERTS)
    chosen = routes.reshape(-1)
    modal_flag = jnp.repeat(modality, 2)
    slot_key = chosen * 2 + modal_flag
    choices = slot_key.shape[0]
    order = jnp.arange(choices, dtype=jnp.int32)
    rank_in = jnp.sum(
        ((slot_key[:, None] == slot_key[None, :]) & (order[None, :] < order[:, None])).astype(jnp.int32), 1
    )
    onehot = slot_key[:, None] == jnp.arange(2 * EXPERTS, dtype=jnp.int32)[None, :]
    limit_of = jnp.sum(jnp.where(onehot, capacity.reshape(1, -1), 0), 1)
    kept_mask = rank_in < limit_of
    column = chosen * slot_count + modal_flag * CAP + rank_in
    column = jnp.where(kept_mask, column, -1).reshape(tok_rows, 2)
    holders = EXPERTS // local_experts
    high = (gate_ints & ~7).astype(jnp.float32) / 1024.0
    low = (gate_ints & 7).astype(jnp.float32) / 1024.0
    per = local_experts * slot_count
    if split_ways == 1 and per % 8 == 0 and hidden_each % HEAD == 0 and width_d % (4 * HEAD) == 0:
        ids = jnp.arange(EXPERTS * slot_count, dtype=jnp.int32)
        hit = column[:, :, None] == ids[None, None, :]
        select = jnp.any(hit, 1).astype(jnp.bfloat16)
        comb_high = jnp.sum(jnp.where(hit, high[:, :, None], 0.0), 1).astype(jnp.bfloat16)
        comb_low = jnp.sum(jnp.where(hit, low[:, :, None], 0.0), 1).astype(jnp.bfloat16)
        table = lax.dot_general(
            select, normed, (((0,), (0,)), ((), ())), preferred_element_type=jnp.float32
        ).astype(jnp.bfloat16)
        back = moe(table.reshape(devices, per, width_d), expert_in, expert_down, local_experts, 4)
        both = jnp.dot(
            jnp.concatenate([comb_high, comb_low], 0),
            back.reshape(devices * per, width_d),
            preferred_element_type=jnp.float32,
        )
        return (attended, (both[:tok_rows] + both[tok_rows:]).astype(jnp.bfloat16))
    slot_ids = jnp.arange(EXPERTS * slot_count, dtype=jnp.int32).reshape(holders, local_experts, slot_count)
    total = jnp.zeros((tok_rows, width_d), jnp.float32)
    for local in range(local_experts):
        ids = slot_ids[:, local].reshape(-1)
        hit = column[:, :, None] == ids[None, None, :]
        select = jnp.any(hit, 1).astype(jnp.bfloat16)
        comb_high = jnp.sum(jnp.where(hit, high[:, :, None], 0.0), 1).astype(jnp.bfloat16)
        comb_low = jnp.sum(jnp.where(hit, low[:, :, None], 0.0), 1).astype(jnp.bfloat16)
        table = lax.dot_general(
            select, normed, (((0,), (0,)), ((), ())), preferred_element_type=jnp.float32
        ).astype(jnp.bfloat16)
        outgoing = jnp.repeat(table.reshape(holders, slot_count, width_d), split_ways, 0)
        arrived = lax.all_to_all(outgoing, "seq", split_axis=0, concat_axis=0, tiled=True)
        rows_in = arrived.reshape(devices * slot_count, width_d)
        first = local * hidden_each
        gate_up = jnp.einsum(
            "kd,dgf->gkf", rows_in, expert_in[:, :, first : first + hidden_each], preferred_element_type=jnp.float32
        )
        active = (jax.nn.silu(gate_up[0]) * gate_up[1]).astype(jnp.bfloat16)
        part = jnp.dot(
            active, expert_down[first : first + hidden_each], preferred_element_type=jnp.float32
        ).astype(jnp.bfloat16)
        returned = lax.all_to_all(
            part.reshape(devices, slot_count, width_d), "seq", split_axis=0, concat_axis=0, tiled=True
        )
        if split_ways > 1:
            returned = jnp.sum(
                returned.reshape(holders, split_ways, slot_count, width_d).astype(jnp.float32), 1
            ).astype(jnp.bfloat16)
        mixed = returned.reshape(holders * slot_count, width_d)
        total = (
            total
            + jnp.dot(comb_high, mixed, preferred_element_type=jnp.float32)
            + jnp.dot(comb_low, mixed, preferred_element_type=jnp.float32)
        )
    return (attended, total.astype(jnp.bfloat16))


def solution(mesh):
    placed = (
        P("seq", None),
        P("seq", None),
        P("seq", None),
        P("seq", None),
        P(None, "seq"),
        P(),
        P(None, None, "seq"),
        P("seq", None),
        P("seq", None),
        P("seq", None),
        P("seq"),
        P(),
    )
    return jax.shard_map(
        body,
        mesh=mesh,
        in_specs=placed,
        out_specs=(P("seq", None), P("seq", None)),
        check_vma=False,
    )
```

```python
import functools
import math
import jax
import jax.numpy as jnp
from jax import lax
from jax.experimental import pallas as pl
from jax.experimental.pallas import tpu as pltpu
from jax.sharding import PartitionSpec as P

HEADS = 20
KV_HEADS = 4
HEAD = 128
WINDOW = 1024
EXPERTS = 64
CAP = 2
MESH = pl.DeviceIdType.MESH


def window_blocks(own, chips_back):
    count = lax.axis_size("seq")
    swap = [(source, source ^ 1) for source in range(count)]
    span = 2 * chips_back
    mine = {0: own}
    prev = lax.ppermute(own, "seq", [(s, s + span) for s in range(count - span)])
    mine[chips_back] = prev
    if count % span == 0:
        place = lax.rem(lax.axis_index("seq"), span) // 2
        for step in range(1, chips_back):
            payload = jnp.where(place + step < chips_back, own, prev)
            turn = [(s, s - s % span + (s % span + 2 * step) % span) for s in range(count)]
            mine[step] = lax.ppermute(payload, "seq", turn)
    else:
        for step in range(1, chips_back):
            mine[step] = lax.ppermute(own, "seq", [(s, s + 2 * step) for s in range(count - 2 * step)])
    other = {step: lax.ppermute(block, "seq", swap) for step, block in mine.items()}
    return mine, other


def attend_kernel(chips_back, rows, q_ref, *refs):
    out_ref = refs[-1]
    blocks = 2 * (chips_back + 1)
    k_refs, v_refs = refs[:blocks], refs[blocks : 2 * blocks]
    me = lax.axis_index("seq")
    core = lax.rem(me, 2)
    keys = jnp.concatenate([ref[...] for ref in k_refs], 0)
    vals = jnp.concatenate([ref[...] for ref in v_refs], 0)
    q_pos = me * rows + lax.broadcasted_iota(jnp.int32, (rows, rows), 0)
    lane = lax.broadcasted_iota(jnp.int32, (rows, rows), 1)
    bias = []
    for half in range(2):
        for step in range(chips_back + 1):
            block = (me - core) - 2 * step + (core if half == 0 else 1 - core)
            k_pos = block * rows + lane
            seen = (k_pos <= q_pos) & (k_pos > q_pos - WINDOW) & (k_pos >= 0)
            bias.append(jnp.where(seen, 0.0, -1e30))
    bias = jnp.concatenate(bias, 1)
    scale = HEAD ** (-0.5) * math.log2(math.e)
    for g in range(HEADS // KV_HEADS):
        q_one = q_ref[:, g * HEAD : (g + 1) * HEAD]
        scores = lax.dot_general(q_one, keys, (((1,), (1,)), ((), ())), preferred_element_type=jnp.float32)
        scores = scores * scale + bias
        weights = jnp.exp2(scores - jnp.max(scores, -1, keepdims=True))
        total = jnp.sum(weights, -1, keepdims=True)
        probs = (weights * (1.0 / total)).astype(jnp.bfloat16)
        mixed = jnp.dot(probs, vals, preferred_element_type=jnp.float32)
        out_ref[:, g * HEAD : (g + 1) * HEAD] = mixed.astype(jnp.bfloat16)


def attend(queries, mine, other, chips_back, part):
    rows = queries.shape[0]
    wide = HEADS // KV_HEADS * HEAD
    ordered = [mine[s] for s in range(chips_back + 1)] + [other[s] for s in range(chips_back + 1)]
    heads = KV_HEADS // 2
    first = part * heads
    k_spec = pl.BlockSpec((rows, HEAD), lambda h: (0, first + h))
    v_spec = pl.BlockSpec((rows, HEAD), lambda h: (0, KV_HEADS + first + h))
    q_spec = pl.BlockSpec((rows, wide), lambda h: (0, first + h))
    span = rows * len(ordered)
    return pl.pallas_call(
        functools.partial(attend_kernel, chips_back, rows),
        grid=(heads,),
        out_shape=jax.ShapeDtypeStruct((rows, heads * wide), jnp.bfloat16),
        in_specs=[q_spec] + [k_spec] * len(ordered) + [v_spec] * len(ordered),
        out_specs=pl.BlockSpec((rows, wide), lambda h: (0, h)),
        cost_estimate=pl.CostEstimate(
            flops=2 * HEADS * rows * span * HEAD, bytes_accessed=4 << 20, transcendentals=HEADS * rows * span // 2
        ),
        name="attend",
    )(queries, *ordered, *ordered)


def project(halves, out_proj):
    count = lax.axis_size("seq")
    flip = [[(source, source ^ bits) for source in range(count)] for bits in range(4)]
    classes = [[s for s in range(count) if s % 4 == kind] for kind in range(4)]
    weights = lax.all_gather(out_proj.T, "seq", axis=0, tiled=True, axis_index_groups=classes)
    far = [lax.ppermute(half, "seq", flip[2]) for half in halves]
    near = [lax.ppermute(half, "seq", flip[1]) for half in halves]
    cross = [lax.ppermute(half, "seq", flip[1]) for half in far]
    return gather_columns(weights, [jnp.concatenate(pieces, 1) for pieces in (halves, near, far, cross)])


def gather_columns(weights, contexts):
    count = lax.axis_size("seq")
    rows = contexts[0].shape[0]
    local = weights.shape[0] * 4 // count
    flip = [[(source, source ^ bits) for source in range(count)] for bits in range(4)]

    def product(context):
        return lax.dot_general(
            weights, context, (((1,), (1,)), ((), ())), preferred_element_type=jnp.float32
        ).astype(jnp.bfloat16)

    part = [None] * 4
    for bits in (2, 3, 1):
        part[bits] = lax.ppermute(product(contexts[bits]), "seq", flip[bits])
    part[0] = product(contexts[0])
    place = lax.axis_index("seq")
    odd = lax.rem(place, 2) == 1
    upper = lax.rem(place, 4) >= 2
    same = [jnp.where(odd, part[1], part[0]), jnp.where(odd, part[0], part[1])]
    away = [jnp.where(odd, part[3], part[2]), jnp.where(odd, part[2], part[3])]
    ordered = [jnp.where(upper, f, e) for e, f in zip(same, away)] + [jnp.where(upper, e, f) for e, f in zip(same, away)]
    columns = jnp.concatenate([piece.reshape(count // 4, local, rows) for piece in ordered], 1)
    return columns.reshape(count * local, rows).T


def moe_kernel(
    devices, locals_, parts, tab_ref, comb_ref, win_ref, wdown_ref, mix_ref,
    ret_ref, arrive, part, wi, wd, acc, spread, act, wi_sem, wd_sem, send_sem, recv_sem, back_send, back_recv,
):
    me = lax.axis_index("seq")
    per, width = tab_ref.shape[1], tab_ref.shape[2]
    step = width // parts
    rows = devices * per
    each = rows // locals_
    blocks = win_ref.shape[1]
    mine = blocks // locals_
    hidden = mine * HEAD
    slots = per // locals_

    def columns(c):
        return pl.ds(pl.multiple_of(c * step, step), step)

    def fetch_in(c, j):
        where = pl.ds(pl.multiple_of(c * step, step), step)
        return pltpu.make_async_copy(win_ref.at[where, j], wi.at[j, where], wi_sem.at[c])

    def all_in(c):
        where = pl.ds(pl.multiple_of(c * step, step), step)
        return pltpu.make_async_copy(wi.at[:, where], wi.at[:, where], wi_sem.at[c])

    fetch_down = pltpu.make_async_copy(wdown_ref, wd, wd_sem)

    barrier = pltpu.get_barrier_semaphore()

    def greet(k, _):
        pl.semaphore_signal(barrier, inc=1, device_id=(lax.rem(me + k, devices),), device_id_type=MESH)
        return 0

    lax.fori_loop(1, devices, greet, 0)
    for c in range(parts):
        lax.fori_loop(0, blocks, lambda j, _: (fetch_in(c, j).start(), 0)[1], 0)
    fetch_down.start()
    pl.semaphore_wait(barrier, devices - 1)

    def dispatch(c):
        def send(k, _):
            peer = lax.rem(me + k, devices)
            pltpu.make_async_remote_copy(
                src_ref=tab_ref.at[peer, :, columns(c)],
                dst_ref=arrive.at[me, :, columns(c)],
                send_sem=send_sem.at[c],
                recv_sem=recv_sem.at[c],
                device_id=(peer,),
                device_id_type=MESH,
            ).start()
            return 0

        lax.fori_loop(1, devices, send, 0)
        pltpu.make_async_copy(tab_ref.at[me, :, columns(c)], arrive.at[me, :, columns(c)], recv_sem.at[c]).start()

    for c in range(parts):
        dispatch(c)

    to = lax.broadcasted_iota(jnp.int32, (rows, rows), 0)
    frm = lax.broadcasted_iota(jnp.int32, (rows, rows), 1)
    group, inner = to // each, to % each
    sort = (frm == (inner // slots) * per + group * slots + inner % slots).astype(jnp.bfloat16)
    source, place = to // per, to % per
    unsort = (frm == (place // slots) * each + source * slots + place % slots).astype(jnp.bfloat16)
    wide = lax.broadcasted_iota(jnp.int32, (HEAD, 2 * HEAD), 1)
    double = (wide // 2 == lax.broadcasted_iota(jnp.int32, (HEAD, 2 * HEAD), 0)).astype(jnp.bfloat16)
    even = lax.broadcasted_iota(jnp.int32, (rows, 2 * HEAD), 1) % 2 == 0

    for c in range(parts):
        cols = slice(c * step, (c + 1) * step)
        pltpu.make_async_copy(arrive.at[:, :, cols], arrive.at[:, :, cols], recv_sem.at[c]).wait()
        got = arrive[:, :, cols].reshape(rows, step)
        got = jnp.dot(sort, got, preferred_element_type=jnp.float32).astype(jnp.bfloat16)
        for t in range(step // HEAD):
            pair = jnp.dot(got[:, t * HEAD : (t + 1) * HEAD], double, preferred_element_type=jnp.float32)
            gate_side = jnp.where(even, pair, 0.0).astype(jnp.bfloat16)
            up_side = jnp.where(even, 0.0, pair).astype(jnp.bfloat16)
            for e in range(locals_):
                lanes = slice(2 * t * HEAD, 2 * (t + 1) * HEAD)
                spread[e, 0:each, lanes] = gate_side[e * each : (e + 1) * each]
                spread[e, each : 2 * each, lanes] = up_side[e * each : (e + 1) * each]
        all_in(c).wait()
        for e in range(locals_):
            left = spread[e]

            def weight(j):
                return wi[e * mine + j, cols].reshape(2 * step, HEAD)

            def two(p, _):
                right = jnp.concatenate([weight(2 * p), weight(2 * p + 1)], 1)
                value = jnp.dot(left, right, preferred_element_type=jnp.float32)
                acc[e, p] = value if c == 0 else acc[e, p] + value
                return 0

            lax.fori_loop(0, mine // 2, two, 0, unroll=2)
            if mine % 2:
                value = jnp.dot(left, weight(mine - 1), preferred_element_type=jnp.float32)
                last = mine // 2
                acc[e, last, :, 0:HEAD] = value if c == 0 else acc[e, last, :, 0:HEAD] + value

    for e in range(locals_):
        for p in range((mine + 1) // 2):
            size = min(2 * HEAD, hidden - 2 * HEAD * p)
            gate, up = acc[e, p, 0:each, 0:size], acc[e, p, each : 2 * each, 0:size]
            act[e, :, 2 * HEAD * p : 2 * HEAD * p + size] = (jax.nn.silu(gate) * up).astype(jnp.bfloat16)

    fetch_down.wait()

    def finish(c, _):
        cols = columns(c)
        pieces = []
        for e in range(locals_):
            pieces.append(
                jnp.dot(
                    act[e], wd[e * hidden : (e + 1) * hidden, cols], preferred_element_type=jnp.float32
                ).astype(jnp.bfloat16)
            )
        out = jnp.dot(unsort, jnp.concatenate(pieces, 0), preferred_element_type=jnp.float32)
        part[:, :, cols] = out.astype(jnp.bfloat16).reshape(devices, per, step)

        def send(k, _):
            peer = lax.rem(me + k, devices)
            pltpu.make_async_remote_copy(
                src_ref=part.at[peer, :, cols],
                dst_ref=ret_ref.at[me, :, cols],
                send_sem=back_send.at[c],
                recv_sem=back_recv.at[c],
                device_id=(peer,),
                device_id_type=MESH,
            ).start()
            return 0

        lax.fori_loop(1, devices, send, 0)
        pltpu.make_async_copy(part.at[me, :, cols], ret_ref.at[me, :, cols], back_recv.at[c]).start()
        return 0

    lax.fori_loop(0, parts, finish, 0)
    tokens = mix_ref.shape[0]
    for c in range(parts):
        cols = slice(c * step, (c + 1) * step)
        pltpu.make_async_copy(ret_ref.at[:, :, cols], ret_ref.at[:, :, cols], back_recv.at[c]).wait()
        back = ret_ref[:, :, cols].reshape(rows, step)
        both = jnp.dot(comb_ref[...], back, preferred_element_type=jnp.float32)
        mix_ref[:, cols] = (both[:tokens] + both[tokens:]).astype(jnp.bfloat16)
    for c in range(parts):
        cols = slice(c * step, (c + 1) * step)
        others = slice(0, devices - 1)
        pltpu.make_async_copy(tab_ref.at[others, :, cols], arrive.at[others, :, cols], send_sem.at[c]).wait()
        pltpu.make_async_copy(part.at[others, :, cols], arrive.at[others, :, cols], back_send.at[c]).wait()


def moe(table, combine, expert_in, expert_down, locals_, parts):
    devices, per, width = table.shape
    blocks = expert_in.shape[2] // HEAD
    mine = blocks // locals_
    step = width // parts
    each = devices * per // locals_
    view = expert_in.reshape(width, 2, blocks, HEAD).transpose(0, 2, 1, 3)
    shape = (devices, per, width)
    return pl.pallas_call(
        functools.partial(moe_kernel, devices, locals_, parts),
        out_shape=jax.ShapeDtypeStruct((combine.shape[0] // 2, width), jnp.bfloat16),
        in_specs=[
            pl.BlockSpec(memory_space=pltpu.VMEM),
            pl.BlockSpec(memory_space=pltpu.VMEM),
            pl.BlockSpec(memory_space=pl.ANY),
            pl.BlockSpec(memory_space=pl.ANY),
        ],
        out_specs=pl.BlockSpec(memory_space=pltpu.VMEM),
        scratch_shapes=[
            pltpu.VMEM(shape, jnp.bfloat16),
            pltpu.VMEM(shape, jnp.bfloat16),
            pltpu.VMEM(shape, jnp.bfloat16),
            pltpu.VMEM((blocks, width, 2, HEAD), jnp.bfloat16),
            pltpu.VMEM(expert_down.shape, jnp.bfloat16),
            pltpu.VMEM((locals_, (mine + 1) // 2, 2 * each, 2 * HEAD), jnp.float32),
            pltpu.VMEM((locals_, 2 * each, 2 * step), jnp.bfloat16),
            pltpu.VMEM((locals_, each, mine * HEAD), jnp.bfloat16),
            pltpu.SemaphoreType.DMA((parts,)),
            pltpu.SemaphoreType.DMA,
            pltpu.SemaphoreType.DMA((parts,)),
            pltpu.SemaphoreType.DMA((parts,)),
            pltpu.SemaphoreType.DMA((parts,)),
            pltpu.SemaphoreType.DMA((parts,)),
        ],
        compiler_params=pltpu.CompilerParams(
            collective_id=0, has_side_effects=True, vmem_limit_bytes=66 * 1024 * 1024 - 2**21
        ),
        cost_estimate=pl.CostEstimate(flops=10**10, bytes_accessed=51 << 20, transcendentals=0),
        name="moe",
    )(table, combine, view, expert_down)


def front_kernel(
    cut, q_any, k_ref, v_ref, w_ref, ctx_ref, wg_ref,
    q_ref, km, vm, ko, vo, bias_ref,
    q_sem, kv_send, mine_sem, other_sem, up_send, down_send, side_send, whole_sem, tail_sem, own_sem, ctx_send, ctx_recv,
):
    count = lax.axis_size("seq")
    me = lax.axis_index("seq")
    rows = q_any.shape[0]
    near_steps = km.shape[0] - 1
    span = 2 * near_steps
    planes = count // span
    local = w_ref.shape[0]
    plane = me // span
    inside = me % span
    place = inside // 2
    core = me % 2
    column = inside // 4
    pal = me + 1 - 2 * core
    across = me + 2 - 4 * (place % 2)
    side = me + 4 - 8 * column
    above, below = me + span, me - span
    has_above, has_below = plane + 1 < planes, plane >= 1

    def remote(src, dst, send, recv, peer):
        return pltpu.make_async_remote_copy(
            src_ref=src, dst_ref=dst, send_sem=send, recv_sem=recv, device_id=(peer,), device_id_type=MESH
        )

    def landed(ref, sem):
        pltpu.make_async_copy(ref, ref, sem).wait()

    load = pltpu.make_async_copy(q_any, q_ref, q_sem)
    load.start()
    barrier = pltpu.get_barrier_semaphore()

    def greet(peer):
        pl.semaphore_signal(barrier, inc=1, device_id=(peer,), device_id_type=MESH)

    def turned(step):
        return me - inside + (inside + 2 * step) % span

    greet(pal)
    for step in range(1, near_steps):
        greet(turned(step))
    pl.when(has_above)(lambda: greet(above))
    pl.when(has_below)(lambda: greet(below))
    pl.semaphore_wait(
        barrier, near_steps + has_above.astype(jnp.int32) + has_below.astype(jnp.int32)
    )

    def kv(src_k, src_v, dst_k, dst_v, lane, recv, peer):
        return [
            remote(src_k, dst_k, kv_send.at[lane, 0], recv.at[0], peer),
            remote(src_v, dst_v, kv_send.at[lane, 1], recv.at[1], peer),
        ]

    def go(copies):
        for copy in copies:
            copy.start()

    def rise():
        return kv(k_ref, v_ref, km.at[near_steps], vm.at[near_steps], 0, mine_sem.at[near_steps], above)

    def turn(step, late):
        a, b = (km.at[near_steps], vm.at[near_steps]) if late else (k_ref, v_ref)
        return kv(a, b, km.at[step], vm.at[step], step, mine_sem.at[step], turned(step))

    def share(step):
        a, b = (km.at[step], vm.at[step]) if step else (k_ref, v_ref)
        return kv(a, b, ko.at[step], vo.at[step], near_steps + step, other_sem.at[step], pal)

    def early(step):
        return (place + step < near_steps) | (plane == 0)

    pl.when(has_above)(lambda: go(rise()))
    for step in range(1, near_steps):
        pl.when(early(step))(lambda step=step: go(turn(step, False)))
    go(share(0))
    go([
        pltpu.make_async_copy(k_ref, km.at[0], mine_sem.at[0, 0]),
        pltpu.make_async_copy(v_ref, vm.at[0], mine_sem.at[0, 1]),
    ])

    @pl.when(plane == 0)
    def _():
        go([
            pltpu.make_async_copy(k_ref, km.at[near_steps], mine_sem.at[near_steps, 0]),
            pltpu.make_async_copy(v_ref, vm.at[near_steps], mine_sem.at[near_steps, 1]),
        ])

    head, tail = pl.ds(0, cut), pl.ds(cut, local - cut)

    def slot(level, col):
        return 2 * level + col

    def lift(hop, upward):
        level = plane - hop if upward else plane + hop
        peer = above if upward else below
        sends = up_send if upward else down_send
        s = slot(level, column)
        src = w_ref if hop == 0 else wg_ref.at[s]
        return remote(src, wg_ref.at[s], sends.at[hop, 0], whole_sem.at[s], peer)

    def lift_tail(hop, upward):
        level = plane - hop if upward else plane + hop
        peer = above if upward else below
        sends = up_send if upward else down_send
        s = slot(level, 1 - column)
        return remote(wg_ref.at[s, tail], wg_ref.at[s, tail], sends.at[hop, 1], tail_sem.at[s], peer)

    def across_side(hop, upward):
        level = plane - hop if upward else plane + hop
        s = slot(level, column)
        src = w_ref.at[head] if hop == 0 else wg_ref.at[s, head]
        return remote(src, wg_ref.at[s, head], side_send.at[level], whole_sem.at[s], side)

    def side_tail():
        s = slot(plane, column)
        return remote(w_ref.at[tail], wg_ref.at[s, tail], side_send.at[planes], tail_sem.at[s], side)

    side_tail().start()
    pl.when(has_above)(lambda: lift(0, True).start())
    pl.when(has_below)(lambda: lift(0, False).start())
    across_side(0, True).start()
    own_slot = slot(plane, column)
    keep = pltpu.make_async_copy(w_ref, wg_ref.at[own_slot], own_sem)
    keep.start()

    def first_tail():
        s = slot(plane, 1 - column)
        landed(wg_ref.at[s, tail], tail_sem.at[s])
        pl.when(has_above)(lambda: lift_tail(0, True).start())
        pl.when(has_below)(lambda: lift_tail(0, False).start())

    def relay(hop):
        for upward in (True, False):
            level = plane - hop if upward else plane + hop
            here = level >= 0 if upward else level < planes
            more = has_above if upward else has_below

            @pl.when(here)
            def _():
                s = slot(level, column)
                landed(wg_ref.at[s], whole_sem.at[s])
                pl.when(more)(lambda: lift(hop, upward).start())
                across_side(hop, upward).start()
                o = slot(level, 1 - column)
                landed(wg_ref.at[o, tail], tail_sem.at[o])
                pl.when(more)(lambda: lift_tail(hop, upward).start())

    def mine_landed(step):
        landed(km.at[step], mine_sem.at[step, 0])
        landed(vm.at[step], mine_sem.at[step, 1])

    q_pos = me * rows + lax.broadcasted_iota(jnp.int32, (rows, rows), 0)
    lane = lax.broadcasted_iota(jnp.int32, (rows, rows), 1)
    for half in range(2):
        for step in range(near_steps + 1):
            block = (me - core) - 2 * step + (core if half == 0 else 1 - core)
            k_pos = block * rows + lane
            seen = (k_pos <= q_pos) & (k_pos > q_pos - WINDOW) & (k_pos >= 0)
            at = (half * (near_steps + 1) + step) * rows
            bias_ref[:, at : at + rows] = jnp.where(seen, 0.0, -1e30)

    mine_landed(near_steps)
    for step in range(1, near_steps):
        pl.when(jnp.logical_not(early(step)))(lambda step=step: go(turn(step, True)))
    go(share(near_steps))
    first_tail()
    mine_landed(0)
    for step in range(1, near_steps):
        mine_landed(step)
        go(share(step))
    relay(1)
    for step in range(near_steps + 1):
        landed(ko.at[step], other_sem.at[step, 0])
        landed(vo.at[step], other_sem.at[step, 1])

    load.wait()
    scale = HEAD ** (-0.5) * math.log2(math.e)
    heads = HEADS // KV_HEADS
    wide = heads * HEAD

    def context(g, peer_kind):
        cols = pl.ds(pl.multiple_of(g * wide, wide), wide)
        peer = pal if peer_kind == 0 else across
        return remote(
            ctx_ref.at[0, :, cols], ctx_ref.at[1 + peer_kind, :, cols],
            ctx_send.at[peer_kind, g], ctx_recv.at[peer_kind, g], peer,
        )

    def passed(g):
        cols = pl.ds(pl.multiple_of(g * wide, wide), wide)
        return remote(ctx_ref.at[2, :, cols], ctx_ref.at[3, :, cols], ctx_send.at[2, g], ctx_recv.at[2, g], pal)

    def group(g, _):
        cols = pl.ds(pl.multiple_of(g * HEAD, HEAD), HEAD)
        keys = jnp.concatenate(
            [ref[s, :, cols] for ref in (km, ko) for s in range(near_steps + 1)], 0
        )
        vals = jnp.concatenate(
            [ref[s, :, cols] for ref in (vm, vo) for s in range(near_steps + 1)], 0
        )
        for h in range(heads):
            at = pl.ds(pl.multiple_of(g * wide + h * HEAD, HEAD), HEAD)
            scores = lax.dot_general(
                q_ref[:, at], keys, (((1,), (1,)), ((), ())), preferred_element_type=jnp.float32
            )
            scores = scores * scale + bias_ref[...]
            weights = jnp.exp2(scores - jnp.max(scores, -1, keepdims=True))
            total = jnp.sum(weights, -1, keepdims=True)
            mixed = jnp.dot(weights.astype(jnp.bfloat16), vals, preferred_element_type=jnp.float32)
            ctx_ref[0, :, at] = (mixed * (1.0 / total)).astype(jnp.bfloat16)
        context(g, 1).start()
        context(g, 0).start()
        pl.when(g == 1)(lambda: relay(2))
        return 0

    lax.fori_loop(0, KV_HEADS, group, 0)
    for hop in range(3, planes):
        relay(hop)

    for g in range(KV_HEADS):
        cols = slice(g * wide, (g + 1) * wide)
        landed(ctx_ref.at[2, :, cols], ctx_recv.at[1, g])
        passed(g).start()
    for level in range(planes):
        s = slot(level, 1 - column)
        landed(wg_ref.at[s, head], whole_sem.at[s])
    keep.wait()
    for g in range(KV_HEADS):
        cols = slice(g * wide, (g + 1) * wide)
        landed(ctx_ref.at[1, :, cols], ctx_recv.at[0, g])
        landed(ctx_ref.at[3, :, cols], ctx_recv.at[2, g])
        context(g, 0).wait_send()
        context(g, 1).wait_send()
        passed(g).wait_send()

    def sent(copies):
        for copy in copies:
            copy.wait_send()

    pl.when(has_above)(lambda: sent(rise()))
    for step in range(1, near_steps):
        sent(turn(step, False))
    for step in range(near_steps + 1):
        sent(share(step))
    sent([side_tail(), across_side(0, True)])
    for upward in (True, False):
        more = has_above if upward else has_below
        pl.when(more)(lambda upward=upward: sent([lift(0, upward), lift_tail(0, upward)]))
        for hop in range(1, planes):
            level = plane - hop if upward else plane + hop
            here = level >= 0 if upward else level < planes
            pl.when(here)(lambda hop=hop, upward=upward: sent([across_side(hop, upward)]))
            pl.when(here & more)(
                lambda hop=hop, upward=upward: sent([lift(hop, upward), lift_tail(hop, upward)])
            )


def front(queries, keys, values, columns, near_steps):
    count = lax.axis_size("seq")
    rows, wide = queries.shape
    span = 2 * near_steps
    planes = count // span
    local = columns.shape[0]
    cut = local * 4 // 5 // 8 * 8
    narrow = keys.shape[1]
    vmem = pl.BlockSpec(memory_space=pltpu.VMEM)
    dma = pltpu.SemaphoreType.DMA
    blocks = pltpu.VMEM((near_steps + 1, rows, narrow), jnp.bfloat16)
    return pl.pallas_call(
        functools.partial(front_kernel, cut),
        out_shape=(
            jax.ShapeDtypeStruct((4, rows, wide), jnp.bfloat16),
            jax.ShapeDtypeStruct((2 * planes, local, wide), jnp.bfloat16),
        ),
        in_specs=[pl.BlockSpec(memory_space=pl.ANY)] * 4,
        out_specs=(vmem, vmem),
        scratch_shapes=[
            pltpu.VMEM((rows, wide), jnp.bfloat16),
            blocks, blocks, blocks, blocks,
            pltpu.VMEM((rows, 2 * (near_steps + 1) * rows), jnp.float32),
            dma,
            dma((2 * near_steps + 1, 2)),
            dma((near_steps + 1, 2)),
            dma((near_steps + 1, 2)),
            dma((planes, 2)),
            dma((planes, 2)),
            dma((planes + 1,)),
            dma((2 * planes,)),
            dma((2 * planes,)),
            dma,
            dma((3, KV_HEADS)),
            dma((3, KV_HEADS)),
        ],
        compiler_params=pltpu.CompilerParams(
            collective_id=1, has_side_effects=True, vmem_limit_bytes=40 * 1024 * 1024
        ),
        cost_estimate=pl.CostEstimate(flops=2 * 10**9, bytes_accessed=8 << 20, transcendentals=0),
        name="front",
    )(queries, keys, values, columns)


def body(
    residual,
    queries,
    keys,
    values,
    out_proj,
    norm_gain,
    expert_in,
    expert_down,
    routes,
    gate_ints,
    modality,
    capacity,
):
    devices = lax.axis_size("seq")
    tok_rows = residual.shape[0]
    width_d = residual.shape[1]
    chips_back = ((WINDOW + tok_rows - 1) // tok_rows + 1) // 2
    local_experts = max(1, EXPERTS // devices)
    hidden_each = expert_in.shape[2] // local_experts
    if devices % (2 * chips_back) == 0 and chips_back == 4 and out_proj.shape[1] % 16 == 0:
        contexts, gathered = front(queries, keys, values, out_proj.T, chips_back)
        weights = gathered.reshape(devices // 4 * out_proj.shape[1], width_d)
        attended = gather_columns(weights, [contexts[bits] for bits in range(4)])
    else:
        mine, other = window_blocks(jnp.concatenate([keys, values], 1), chips_back)
        halves = [attend(queries, mine, other, chips_back, part) for part in range(2)]
        attended = project(halves, out_proj)
    attended = lax.optimization_barrier(attended)
    hidden = residual.astype(jnp.float32) + attended.astype(jnp.float32)
    normed = (
        hidden * lax.rsqrt(jnp.mean(hidden * hidden, -1, keepdims=True) + 1e-05) * norm_gain
    ).astype(jnp.bfloat16)
    slot_count = 2 * CAP
    split_ways = max(1, devices // EXPERTS)
    chosen = routes.reshape(-1)
    modal_flag = jnp.repeat(modality, 2)
    slot_key = chosen * 2 + modal_flag
    choices = slot_key.shape[0]
    order = jnp.arange(choices, dtype=jnp.int32)
    rank_in = jnp.sum(
        ((slot_key[:, None] == slot_key[None, :]) & (order[None, :] < order[:, None])).astype(jnp.int32), 1
    )
    onehot = slot_key[:, None] == jnp.arange(2 * EXPERTS, dtype=jnp.int32)[None, :]
    limit_of = jnp.sum(jnp.where(onehot, capacity.reshape(1, -1), 0), 1)
    kept_mask = rank_in < limit_of
    column = chosen * slot_count + modal_flag * CAP + rank_in
    column = jnp.where(kept_mask, column, -1).reshape(tok_rows, 2)
    holders = EXPERTS // local_experts
    high = (gate_ints & ~7).astype(jnp.float32) / 1024.0
    low = (gate_ints & 7).astype(jnp.float32) / 1024.0
    per = local_experts * slot_count
    if split_ways == 1 and per % 8 == 0 and hidden_each % HEAD == 0 and width_d % (4 * HEAD) == 0:
        ids = jnp.arange(EXPERTS * slot_count, dtype=jnp.int32)
        hit = column[:, :, None] == ids[None, None, :]
        select = jnp.any(hit, 1).astype(jnp.bfloat16)
        comb_high = jnp.sum(jnp.where(hit, high[:, :, None], 0.0), 1).astype(jnp.bfloat16)
        comb_low = jnp.sum(jnp.where(hit, low[:, :, None], 0.0), 1).astype(jnp.bfloat16)
        table = lax.dot_general(
            select, normed, (((0,), (0,)), ((), ())), preferred_element_type=jnp.float32
        ).astype(jnp.bfloat16)
        combine = jnp.concatenate([comb_high, comb_low], 0)
        mix = moe(table.reshape(devices, per, width_d), combine, expert_in, expert_down, local_experts, 4)
        return (attended, mix)
    slot_ids = jnp.arange(EXPERTS * slot_count, dtype=jnp.int32).reshape(holders, local_experts, slot_count)
    total = jnp.zeros((tok_rows, width_d), jnp.float32)
    for local in range(local_experts):
        ids = slot_ids[:, local].reshape(-1)
        hit = column[:, :, None] == ids[None, None, :]
        select = jnp.any(hit, 1).astype(jnp.bfloat16)
        comb_high = jnp.sum(jnp.where(hit, high[:, :, None], 0.0), 1).astype(jnp.bfloat16)
        comb_low = jnp.sum(jnp.where(hit, low[:, :, None], 0.0), 1).astype(jnp.bfloat16)
        table = lax.dot_general(
            select, normed, (((0,), (0,)), ((), ())), preferred_element_type=jnp.float32
        ).astype(jnp.bfloat16)
        outgoing = jnp.repeat(table.reshape(holders, slot_count, width_d), split_ways, 0)
        arrived = lax.all_to_all(outgoing, "seq", split_axis=0, concat_axis=0, tiled=True)
        rows_in = arrived.reshape(devices * slot_count, width_d)
        first = local * hidden_each
        gate_up = jnp.einsum(
            "kd,dgf->gkf", rows_in, expert_in[:, :, first : first + hidden_each], preferred_element_type=jnp.float32
        )
        active = (jax.nn.silu(gate_up[0]) * gate_up[1]).astype(jnp.bfloat16)
        part = jnp.dot(
            active, expert_down[first : first + hidden_each], preferred_element_type=jnp.float32
        ).astype(jnp.bfloat16)
        returned = lax.all_to_all(
            part.reshape(devices, slot_count, width_d), "seq", split_axis=0, concat_axis=0, tiled=True
        )
        if split_ways > 1:
            returned = jnp.sum(
                returned.reshape(holders, split_ways, slot_count, width_d).astype(jnp.float32), 1
            ).astype(jnp.bfloat16)
        mixed = returned.reshape(holders * slot_count, width_d)
        total = (
            total
            + jnp.dot(comb_high, mixed, preferred_element_type=jnp.float32)
            + jnp.dot(comb_low, mixed, preferred_element_type=jnp.float32)
        )
    return (attended, total.astype(jnp.bfloat16))


def solution(mesh):
    placed = (
        P("seq", None),
        P("seq", None),
        P("seq", None),
        P("seq", None),
        P(None, "seq"),
        P(),
        P(None, None, "seq"),
        P("seq", None),
        P("seq", None),
        P("seq", None),
        P("seq"),
        P(),
    )
    return jax.shard_map(
        body,
        mesh=mesh,
        in_specs=placed,
        out_specs=(P("seq", None), P("seq", None)),
        check_vma=False,
    )
```
